256 devices in a mesh: rows: 16 (over x, y_hi, core), mp: 16 (over y_lo, z).
Axes of the slice: x: 4, y: 4 (y_hi: 2, y_lo: 2; y = y_hi * 2 + y_lo), z: 8, core: 2. Of those that a mesh axis runs over, the one named last changes fastest.
Arguments:
- tokens: bfloat16 [2048, 3584], P('rows', 'mp'), may hold values from -6 to 6
- modality: int32 [2048], replicated, may hold values from 0 to 1, as said below
- attn_gain: float32 [2, 3584], P(None, 'mp'), may hold values from 0.1 to 1.9
- ffn_gain: float32 [2, 3584], P(None, 'mp'), may hold values from 0.1 to 1.9
- w_query: bfloat16 [2, 3584, 2048], P(None, 'mp', 'rows'), may hold values from -4 to 4
- w_keyval: bfloat16 [2, 3584, 1024], P(None, 'mp', 'rows'), may hold values from -4 to 4
- w_out: bfloat16 [2, 2048, 3584], P(None, 'rows', 'mp'), may hold values from -0.125 to 0.125
- w_gate: bfloat16 [2, 3584, 9472], P(None, 'mp', 'rows'), may hold values from -0.09375 to 0.09375
- w_up: bfloat16 [2, 3584, 9472], P(None, 'mp', 'rows'), may hold values from -0.09375 to 0.09375
- w_down: bfloat16 [2, 9472, 3584], P(None, 'rows', 'mp'), may hold values from -0.0625 to 0.0625
Outputs:
- mixed: bfloat16 [2048, 3584], P('rows', 'mp')
The draws below stay inside these ranges and needn't reach their ends.
Inputs may be any that keep to these rules, and one draw needn't show every extreme that they name: `modality`: constant over each aligned block of 128 positions.
All inputs are finite; a program needn't handle non-finite values.
Results may differ from the reference program's by a relative error of at most 0.024.
Values may be sent and summed in bfloat16 or wider, within the bound.
A program may use at most 64 MiB of HBM per device.

```python
import jax
import jax.numpy as jnp
from jax import lax

D = 3584
FF = 9472
HD = 128
KV = 4
HEADS = 16
MODAL_BLOCK = 128
TOKENS = 2048
N_MP = 16


def paired_weights(key):
    key_weights = jax.random.normal(jax.random.fold_in(key, 1102), (2, D, KV * HD), jnp.float32) * D ** (-0.5)
    value_weights = jax.random.normal(jax.random.fold_in(key, 1103), (2, D, KV * HD), jnp.float32) * D ** (-0.5)
    return (key_weights, value_weights)


def draw_w_keyval(key, part):
    key_weights, value_weights = paired_weights(key)
    joined = jnp.concatenate((key_weights, value_weights), axis=2)
    return jnp.clip(joined, -4.0, 4.0).astype(jnp.bfloat16)


def draw_w_query(key, part):
    noise_part = jax.random.normal(jax.random.fold_in(key, 1104), (2, D, HEADS * HD), jnp.float32) * D ** (-0.5)
    blended = noise_part
    return jnp.clip(blended, -4.0, 4.0).astype(jnp.bfloat16)


def draw_modality(key, part):
    block_ids = jax.random.randint(jax.random.fold_in(key, 1201), (TOKENS // MODAL_BLOCK,), 0, 2)
    return jnp.repeat(block_ids, MODAL_BLOCK).astype(jnp.int32)


def steps_of(key, dims, cuts, least, high):
    factor_of = 1.0
    for axis_at, blocks in cuts:
        draws = jax.random.uniform(jax.random.fold_in(jax.random.fold_in(key, 6), axis_at), (blocks,), jnp.float32, least / len(cuts), high / len(cuts))
        factor_of = factor_of * jnp.repeat(jnp.exp(draws), dims[axis_at] // blocks).reshape((-1,) + (1,) * (len(dims) - 1 - axis_at))
    return factor_of


def noise(key, shape, scale, limit, cuts=(), kind=jnp.bfloat16):
    level = steps_of(key, shape, cuts, -0.22, 0.18) if cuts else 1.0
    values = jax.random.normal(key, shape, jnp.float32) * scale * level
    return jnp.minimum(jnp.maximum(values, -limit), limit).astype(kind)


def setup_inputs(seed: int = 0) -> dict:
    seeds = jax.random.split(jax.random.key(seed), 11)
    tokens = noise(seeds[0], (TOKENS, D), 1.0, 6.0, ((0, 16), (1, 16)))
    modality = draw_modality(jax.random.fold_in(seeds[10], 71), 0)
    attn_gain = jnp.clip(1.0 + 0.18 * jax.random.normal(seeds[2], (2, D), jnp.float32), 0.1, 1.9)
    ffn_gain = jnp.clip(1.0 + 0.18 * jax.random.normal(seeds[3], (2, D), jnp.float32), 0.1, 1.9)
    w_query = draw_w_query(jax.random.fold_in(seeds[10], 71), 0)
    w_keyval = draw_w_keyval(jax.random.fold_in(seeds[10], 71), 0)
    w_out = noise(seeds[6], (2, HEADS * HD, D), (HEADS * HD) ** -0.5, 0.125, ((1, 16), (2, 16)))
    w_gate = noise(seeds[7], (2, D, FF), D ** -0.5, 0.09375, ((1, 16), (2, 16)))
    w_up = noise(seeds[8], (2, D, FF), D ** -0.5, 0.09375, ((1, 16), (2, 16)))
    w_down = noise(seeds[9], (2, FF, D), FF ** -0.5, 0.0625, ((1, 16), (2, 16)))
    return {"tokens": tokens, "modality": modality, "attn_gain": attn_gain, "ffn_gain": ffn_gain, "w_query": w_query, "w_keyval": w_keyval, "w_out": w_out, "w_gate": w_gate, "w_up": w_up, "w_down": w_down}


EPSILON = 1e-06

def tower_rows(matrix, weights, tower_ids):
    blocks = matrix.reshape(tower_ids.shape[0], -1, matrix.shape[1])

    def single(item):
        block_rows, tower_id = item
        chosen = lax.dynamic_index_in_dim(weights, tower_id, 0, keepdims=False)
        return jnp.dot(block_rows, chosen, preferred_element_type=jnp.float32)
    return lax.map(single, (blocks, tower_ids)).reshape(matrix.shape[0], -1)

def norm_rows(hidden, gains, modality):
    squares = lax.optimization_barrier(jnp.mean(hidden * hidden, axis=1, keepdims=True))
    chosen = jnp.where(modality[:, None] == 1, gains[1][None, :], gains[0][None, :])
    return (hidden * lax.rsqrt(squares + EPSILON) * chosen).astype(jnp.bfloat16)

def sliced_sum(normed, weights, tower_ids):
    width = normed.shape[1] // N_MP
    summed = jnp.zeros((normed.shape[0], weights.shape[2]), jnp.float32)
    for piece_index in range(N_MP):
        lower = piece_index * width
        term = tower_rows(normed[:, lower:lower + width], weights[:, lower:lower + width, :], tower_ids)
        rounded = lax.optimization_barrier(term.astype(jnp.bfloat16))
        summed = summed + rounded.astype(jnp.float32)
    return summed

def reference(tokens, modality, attn_gain, ffn_gain, w_query, w_keyval, w_out, w_gate, w_up, w_down):
    tower_ids = modality.reshape(-1, MODAL_BLOCK)[:, 0]
    hidden = tokens.astype(jnp.float32)
    normed = norm_rows(hidden, attn_gain, modality)
    queries = tower_rows(normed, w_query, tower_ids).astype(jnp.bfloat16)
    keyvals = tower_rows(normed, w_keyval, tower_ids).astype(jnp.bfloat16)
    positions = jnp.arange(TOKENS, dtype=jnp.int32)
    allowed = positions[None, :] <= positions[:, None]

    def one_head(head):
        head_group = head // (HEADS // KV)
        query = lax.dynamic_slice_in_dim(queries, head * HD, HD, 1)
        key_part = lax.dynamic_slice_in_dim(keyvals, head_group * HD, HD, 1)
        value_part = lax.dynamic_slice_in_dim(keyvals, KV * HD + head_group * HD, HD, 1)
        scores = jnp.dot(query, key_part.T, preferred_element_type=jnp.float32) * HD ** (-0.5)
        scores = jnp.where(allowed, scores, -1e+30)
        largest = lax.optimization_barrier(jnp.max(scores, axis=1, keepdims=True))
        powers = jnp.exp(scores - largest)
        probs = (powers / lax.optimization_barrier(jnp.sum(powers, axis=1, keepdims=True))).astype(jnp.bfloat16)
        return jnp.dot(probs, value_part, preferred_element_type=jnp.float32).astype(jnp.bfloat16)
    context = lax.map(one_head, jnp.arange(HEADS, dtype=jnp.int32))
    context = jnp.transpose(context, (1, 0, 2)).reshape(TOKENS, HEADS * HD)
    residual = hidden + tower_rows(context, w_out, tower_ids)
    normed_ffn = norm_rows(residual, ffn_gain, modality)
    gate = sliced_sum(normed_ffn, w_gate, tower_ids)
    up_sum = sliced_sum(normed_ffn, w_up, tower_ids)
    activated = (jax.nn.silu(gate) * up_sum).astype(jnp.bfloat16)
    mixed = residual + tower_rows(activated, w_down, tower_ids)
    return mixed.astype(jnp.bfloat16)
```

```python
import functools

import jax
import jax.numpy as jnp
from jax import lax
from jax.experimental import pallas as pl
from jax.experimental.pallas import tpu as pltpu
from jax.sharding import Mesh
from jax.sharding import PartitionSpec as P

D = 3584
HD = 128
KV = 4
HEADS = 16
MODAL_BLOCK = 128
ROWS = ("x", "yh", "c")
MP = ("yl", "z")
AXES = ("x", "yh", "c", "yl", "z")
NX, NYH, NZ = 4, 2, 8
NB = NX * NYH

EPSILON = 1e-06
F32 = jnp.float32
BF16 = jnp.bfloat16


def from_everyone(value, axis):
    copies = jnp.broadcast_to(value, (lax.axis_size(axis), *value.shape))
    return lax.all_to_all(copies, axis, split_axis=0, concat_axis=0, tiled=True)


def over_copies(value, axis):
    everything = from_everyone(value, axis)
    return jnp.sum(everything, axis=0)


def laid_out(blocks, dim):
    shape = list(blocks.shape[1:])
    shape[dim] *= blocks.shape[0]
    return jnp.moveaxis(blocks, 0, dim).reshape(shape)


def gather_directly(value, axis, dim):
    return laid_out(from_everyone(value, axis), dim)


def cut_along(value, dim, peers):
    shape = value.shape
    blocks = value.reshape(*shape[:dim], peers, shape[dim] // peers, *shape[dim + 1 :])
    return jnp.moveaxis(blocks, dim, 0)


def sent_and_summed(value, axis, dim):
    blocks = cut_along(value, dim, lax.axis_size(axis))
    arrived = lax.all_to_all(blocks, axis, split_axis=0, concat_axis=0, tiled=True)
    return arrived.astype(jnp.float32).sum(axis=0)


def tower_rows(matrix, weights, tower_ids):
    per_block = matrix.shape[0] // tower_ids.shape[0]
    token_towers = jnp.repeat(tower_ids, per_block)
    is_image = (token_towers == 1)[:, None]
    nothing = jnp.zeros((), matrix.dtype)
    text_rows = jnp.where(is_image, nothing, matrix)
    image_rows = jnp.where(is_image, matrix, nothing)
    text_part = jnp.dot(text_rows, weights[0], preferred_element_type=jnp.float32)
    image_part = jnp.dot(image_rows, weights[1], preferred_element_type=jnp.float32)
    return text_part + image_part


def block_towers(modality):
    return modality.reshape(-1, MODAL_BLOCK)[:, 0]


def scaled_rows(hidden, squares, gains, token_towers):
    inverse = lax.rsqrt(squares / D + EPSILON)
    chosen = jnp.where(token_towers[:, None] == 1, gains[1][None, :], gains[0][None, :])
    return (hidden * inverse[:, None] * chosen).astype(jnp.bfloat16)


def pick_group(matrix, head_group):
    key_part = lax.dynamic_slice_in_dim(matrix, head_group * HD, HD, 1)
    value_part = lax.dynamic_slice_in_dim(matrix, KV * HD + head_group * HD, HD, 1)
    return jnp.concatenate((key_part, value_part), axis=1)


class Place:
    def __init__(self):
        self.at = {a: lax.axis_index(a) for a in AXES}
        self.x, self.h, self.c, self.l, self.z = (self.at[a] for a in AXES)
        self.same = 1 - (self.c - self.l) * (self.c - self.l)

    def id(self, **moved):
        return tuple(moved.get(a, self.at[a]) for a in AXES)

    def cross(self, dx, dh):
        return self.id(
            x=lax.rem(self.x + dx, NX), yh=lax.rem(self.h + dh, NYH), c=self.l, yl=self.c
        )

    def ahead(self, dx, dh):
        return NYH * lax.rem(self.x + dx, NX) + lax.rem(self.h + dh, NYH)

    def behind(self, dx, dh):
        return NYH * lax.rem(self.x - dx + NX, NX) + lax.rem(self.h - dh + NYH, NYH)

    def partner(self):
        return self.id(c=1 - self.c)

    def along(self, k):
        return lax.rem(self.z + k + NZ, NZ)


OFFSETS = tuple((dx, dh) for dx in (2, 1, 3, 0) for dh in (1, 0))


def sent(src, dst, send, recv, target):
    return pltpu.make_async_remote_copy(
        src_ref=src,
        dst_ref=dst,
        send_sem=send,
        recv_sem=recv,
        device_id=target,
        device_id_type=pl.DeviceIdType.MESH,
    )


def greet(place, peers):
    barrier = pltpu.get_barrier_semaphore()
    for peer in peers:
        pl.semaphore_signal(barrier, 1, device_id=peer, device_id_type=pl.DeviceIdType.MESH)
    count = len(peers)
    for dx, dh in OFFSETS:
        if (dx, dh) != (0, 0):
            pl.semaphore_signal(
                barrier, 1, device_id=place.cross(dx, dh), device_id_type=pl.DeviceIdType.MESH
            )
            count += 1

    @pl.when(place.c != place.l)
    def _():
        pl.semaphore_signal(
            barrier, 1, device_id=place.cross(0, 0), device_id_type=pl.DeviceIdType.MESH
        )

    pl.semaphore_wait(barrier, count + 1 - place.same)


def gather_rows(place, src, xg, sems):
    send, recv, fsend, frecv = (sems.at[k] for k in range(4))
    own = NYH * place.x + place.h
    for i, (dx, dh) in enumerate(OFFSETS):
        copy = sent(src, xg.at[place.l, own], send.at[i], recv.at[i], place.cross(dx, dh))
        if (dx, dh) != (0, 0):
            copy.start()
        else:
            pl.when(place.c != place.l)(copy.start)

            @pl.when(place.c == place.l)
            def _():
                xg[place.l, own] = src[...]

    order = sorted(range(NB), key=lambda i: (min(OFFSETS[i][0], NX - OFFSETS[i][0]), OFFSETS[i][1]))
    for i in order:
        dx, dh = OFFSETS[i]
        slot = xg.at[place.c, place.behind(dx, dh)]
        arrive = sent(slot, slot, send.at[i], recv.at[i], place.cross(dx, dh))
        if (dx, dh) != (0, 0):
            arrive.wait_recv()
        else:
            pl.when(place.c != place.l)(arrive.wait_recv)
        sent(slot, slot, fsend.at[i], frecv.at[i], place.partner()).start()
    for i in order:
        dx, dh = OFFSETS[i]
        slot = xg.at[1 - place.c, place.behind(dx, dh)]
        sent(slot, slot, fsend.at[i], frecv.at[i], place.partner()).wait_recv()


def gather_rows_end(place, src, xg, sems):
    send, recv, fsend, frecv = (sems.at[k] for k in range(4))
    for i, (dx, dh) in enumerate(OFFSETS):
        copy = sent(src, src, send.at[i], recv.at[i], place.cross(dx, dh))
        if (dx, dh) != (0, 0):
            copy.wait_send()
        else:
            pl.when(place.c != place.l)(copy.wait_send)
        slot = xg.at[place.c, place.behind(dx, dh)]
        sent(slot, slot, fsend.at[i], frecv.at[i], place.partner()).wait_send()


def reduce_rows(place, part, dbuf, rbuf, sems):
    send, recv, fsend, frecv = (sems.at[k] for k in range(4))
    own = NYH * place.x + place.h
    for i, (dx, dh) in enumerate(OFFSETS):
        j = place.ahead(dx, dh)
        sent(
            part.at[1 - place.c, j], dbuf.at[j], fsend.at[i], frecv.at[i], place.partner()
        ).start()
    for i, (dx, dh) in enumerate(OFFSETS):
        j = place.ahead(dx, dh)
        sent(part.at[1 - place.c, j], dbuf.at[j], fsend.at[i], frecv.at[i], place.partner()).wait_recv()
        total = part[place.c, j].astype(F32) + dbuf[j].astype(F32)
        dbuf[j] = total.astype(BF16)
        copy = sent(dbuf.at[j], rbuf.at[i], send.at[i], recv.at[i], place.cross(dx, dh))
        if (dx, dh) != (0, 0):
            copy.start()
        else:
            pl.when(place.c != place.l)(copy.start)

            @pl.when(place.c == place.l)
            def _():
                rbuf[i] = dbuf[own]

    total = None
    order = sorted(range(NB), key=lambda i: (min(OFFSETS[i][0], NX - OFFSETS[i][0]), OFFSETS[i][1]))
    for i in order:
        dx, dh = OFFSETS[i]
        arrive = sent(rbuf.at[i], rbuf.at[i], send.at[i], recv.at[i], place.cross(dx, dh))
        if (dx, dh) != (0, 0):
            arrive.wait_recv()
        else:
            pl.when(place.c != place.l)(arrive.wait_recv)
        term = rbuf[i].astype(F32)
        total = term if total is None else total + term
    for i, (dx, dh) in enumerate(OFFSETS):
        j = place.ahead(dx, dh)
        sent(part.at[1 - place.c, j], dbuf.at[j], fsend.at[i], frecv.at[i], place.partner()).wait_send()
        copy = sent(dbuf.at[j], rbuf.at[i], send.at[i], recv.at[i], place.cross(dx, dh))
        if (dx, dh) != (0, 0):
            copy.wait_send()
        else:
            pl.when(place.c != place.l)(copy.wait_send)
    return total


PARTS = 4


def sum_along_z(place, partial, pbuf, chain, sems):
    part_rows = MODAL_BLOCK // PARTS
    sides = (1, -1)

    def rows(q):
        return pl.ds(q * part_rows, part_rows)

    def hops(side, q):
        long = (q < PARTS // 2) == (side == 0)
        return 4 if long else 3

    def link(side, k, q, src):
        return sent(
            src,
            chain.at[side, k - 1, :, rows(q), :],
            sems.at[0, side, k - 1, q],
            sems.at[1, side, k - 1, q],
            place.id(z=place.along(sides[side])),
        )

    partial(place.along(4))
    for q in range(PARTS):
        for side in range(2):
            if hops(side, q) == 4:
                link(side, 4, q, pbuf.at[place.along(4), :, rows(q), :]).start()
    for k in (3, 2, 1):
        for side in range(2):
            partial(place.along(k * sides[side]))
            if k == 3:
                j = place.along(k * sides[side])
                for q in range(PARTS):
                    if hops(side, q) == 3:
                        link(side, 3, q, pbuf.at[j, :, rows(q), :]).start()
        for q in range(PARTS):
            for side in range(2):
                j = place.along(k * sides[side])
                if hops(side, q) == 3 and k == 3:
                    continue
                slot = chain.at[side, k, :, rows(q), :]
                link(side, k + 1, q, slot).wait_recv()
                chain[side, k, :, rows(q), :] = (
                    chain[side, k, :, rows(q), :].astype(F32) + pbuf[j, :, rows(q), :].astype(F32)
                ).astype(BF16)
                link(side, k, q, slot).start()
    partial(place.z)
    for q in range(PARTS):
        for side in range(2):
            slot = chain.at[side, 0, :, rows(q), :]
            link(side, 1, q, slot).wait_recv()
    for q in range(PARTS):
        for side in range(2):
            for k in range(1, hops(side, q) + 1):
                link(side, k, q, chain.at[side, k - 1, :, rows(q), :]).wait_send()


def spread_along_z(place, blocks, sems, on_arrival):
    half = MODAL_BLOCK // 2
    sides = (1, -1)

    def link(side, k, q, owner):
        rows = blocks.at[owner, pl.ds(q * half, half), :]
        return sent(
            rows, rows, sems.at[0, side, k - 1, q], sems.at[1, side, k - 1, q],
            place.id(z=place.along(sides[side])),
        )

    def used(side, k, q):
        return k < 4 or q == side

    for q in range(2):
        for side in range(2):
            link(side, 1, q, place.z).start()
    on_arrival(place.z)
    for k in (1, 2, 3, 4):
        for q in range(2):
            for side in range(2):
                if used(side, k, q):
                    owner = place.along(-k * sides[side])
                    link(side, k, q, owner).wait_recv()
                    if k < 4 and used(side, k + 1, q):
                        link(side, k + 1, q, owner).start()
        if k < 4:
            for side in range(2):
                on_arrival(place.along(-k * sides[side]))
        else:
            on_arrival(place.along(4))
    for k in (1, 2, 3, 4):
        for q in range(2):
            for side in range(2):
                if used(side, k, q):
                    link(side, k, q, place.along(-(k - 1) * sides[side])).wait_send()


def as_row(column):
    return jnp.transpose(jnp.broadcast_to(column, (MODAL_BLOCK, MODAL_BLOCK)))[:8]


def as_column(row):
    return jnp.transpose(jnp.broadcast_to(row, (MODAL_BLOCK, MODAL_BLOCK)))[:, :1]


def ffn_kernel(
    towers,
    residual,
    gain_own,
    gain_other,
    gate_own,
    gate_other,
    up_own,
    up_other,
    down_own,
    down_other,
    out,
    src,
    xg,
    wg0,
    wg1,
    wu0,
    wu1,
    wd0,
    wd1,
    pbuf,
    chain,
    ssp,
    ssr,
    acts,
    part,
    dbuf,
    rbuf,
    wsem,
    gsem,
    csem,
    ssem,
    asem,
    rsem,
):
    place = Place()
    loads = [
        pltpu.make_async_copy(a, b, wsem.at[k])
        for k, (a, b) in enumerate(
            ((gate_own, wg0), (gate_other, wg1), (up_own, wu0), (up_other, wu1), (down_own, wd0), (down_other, wd1))
        )
    ]
    for load in loads:
        load.start()
    src[...] = residual[...].astype(BF16)
    greet(place, [place.partner()] + [place.id(z=place.along(k)) for k in range(1, NZ)])
    gather_rows(place, src, xg, gsem)
    for load in loads[:4]:
        load.wait()

    def squares_to(k):
        j = place.along(k)
        return sent(
            ssp.at[j], ssr.at[place.z], ssem.at[0, k], ssem.at[1, k], place.id(z=j)
        )

    def partial(j):
        tower = towers[2 * j + place.l]
        x0 = xg[place.l, j].astype(F32)
        x1 = xg[1 - place.l, j].astype(F32)
        ssp[j] = as_row(
            jnp.sum(x0 * x0, axis=1, keepdims=True) + jnp.sum(x1 * x1, axis=1, keepdims=True)
        )
        n0 = (x0 * gain_own[tower]).astype(BF16)
        n1 = (x1 * gain_other[tower]).astype(BF16)
        for side, (w0, w1) in enumerate(((wg0, wg1), (wu0, wu1))):
            pbuf[j, side] = (
                jnp.dot(n0, w0[tower], preferred_element_type=F32)
                + jnp.dot(n1, w1[tower], preferred_element_type=F32)
            ).astype(BF16)

    sum_along_z(place, partial, pbuf, chain, csem)
    for k in range(1, NZ):
        squares_to(k).start()
    both = (
        pbuf[place.z].astype(F32) + chain[0, 0].astype(F32) + chain[1, 0].astype(F32)
    )
    squares = ssp[place.z]
    for k in range(1, NZ):
        slot = ssr.at[place.along(-k)]
        sent(slot, slot, ssem.at[0, k], ssem.at[1, k], place.id(z=place.along(k))).wait_recv()
        squares = squares + ssr[place.along(-k)]
    scale = as_column(lax.rsqrt(squares[:1] / D + EPSILON))
    gate = both[0] * scale
    up = both[1] * scale
    acts[place.z] = (gate / (1.0 + jnp.exp(-gate)) * up).astype(BF16)
    for load in loads[4:]:
        load.wait()

    def downward(j):
        tower = towers[2 * j + place.l]
        act = acts[j]
        part[place.l, j] = jnp.dot(act, wd0[tower], preferred_element_type=F32).astype(BF16)
        part[1 - place.l, j] = jnp.dot(act, wd1[tower], preferred_element_type=F32).astype(BF16)

    spread_along_z(place, acts, asem, downward)
    total = reduce_rows(place, part, dbuf, rbuf, rsem)
    out[...] = (residual[...] + total).astype(BF16)
    gather_rows_end(place, src, xg, gsem)
    for k in range(1, NZ):
        squares_to(k).wait_send()


def ffn(towers, residual, gains, gate, up, down):
    def other(value):
        return lax.ppermute(value, "yl", [(0, 1), (1, 0)])

    gains = gains[:, None, :]
    width = gate.shape[2]
    feats = gate.shape[1]
    vmem = pl.BlockSpec(memory_space=pltpu.VMEM)
    hbm = pl.BlockSpec(memory_space=pltpu.HBM)
    smem = pl.BlockSpec(memory_space=pltpu.SMEM)
    dma = pltpu.SemaphoreType.DMA
    return pl.pallas_call(
        ffn_kernel,
        out_shape=jax.ShapeDtypeStruct((MODAL_BLOCK, feats), BF16),
        in_specs=[smem, vmem, vmem, vmem] + [hbm] * 6,
        out_specs=vmem,
        scratch_shapes=[
            pltpu.VMEM((MODAL_BLOCK, feats), BF16),
            pltpu.VMEM((2, NB, MODAL_BLOCK, feats), BF16),
            pltpu.VMEM((2, feats, width), BF16),
            pltpu.VMEM((2, feats, width), BF16),
            pltpu.VMEM((2, feats, width), BF16),
            pltpu.VMEM((2, feats, width), BF16),
            pltpu.VMEM((2, width, feats), BF16),
            pltpu.VMEM((2, width, feats), BF16),
            pltpu.VMEM((NZ, 2, MODAL_BLOCK, width), BF16),
            pltpu.VMEM((2, 4, 2, MODAL_BLOCK, width), BF16),
            pltpu.VMEM((NZ, 8, MODAL_BLOCK), F32),
            pltpu.VMEM((NZ, 8, MODAL_BLOCK), F32),
            pltpu.VMEM((NZ, MODAL_BLOCK, width), BF16),
            pltpu.VMEM((2, NB, MODAL_BLOCK, feats), BF16),
            pltpu.VMEM((NB, MODAL_BLOCK, feats), BF16),
            pltpu.VMEM((NB, MODAL_BLOCK, feats), BF16),
            dma((6,)),
            dma((4, NB)),
            dma((2, 2, 4, PARTS)),
            dma((2, NZ)),
            dma((2, 2, 4, 2)),
            dma((4, NB)),
        ],
        compiler_params=pltpu.CompilerParams(collective_id=0, has_side_effects=True),
        name="ffn",
    )(towers, residual, gains, other(gains), gate, other(gate), up, other(up), down, other(down))


def local(tokens, modality, attn_gain, ffn_gain, w_query, w_keyval, w_out, w_gate, w_up, w_down):
    row_count = tokens.shape[0]
    total_rows = row_count * lax.axis_size(ROWS)
    share_rows = total_rows // lax.axis_size(MP)
    row_index = lax.axis_index(ROWS)
    mp_index = lax.axis_index(MP)
    own_towers = lax.dynamic_slice_in_dim(modality, row_index * row_count, row_count)
    hidden = tokens.astype(jnp.float32)
    squares = over_copies(jnp.sum(hidden * hidden, axis=1), MP)
    normed = scaled_rows(hidden, squares, attn_gain, own_towers)
    normed_all = gather_directly(normed, ROWS, 0)
    joint_weight = jnp.concatenate((w_query, w_keyval), axis=2)
    picked = normed_all
    projected = sent_and_summed(
        tower_rows(picked, joint_weight, block_towers(modality)).astype(jnp.bfloat16), MP, 0
    ).astype(jnp.bfloat16)
    query_width = w_query.shape[2]
    heads_here = query_width // HD
    queries = projected[:, :query_width].reshape(share_rows, heads_here, HD)
    keyval_local = projected[:, query_width:]
    head_group = row_index * heads_here // (HEADS // KV)
    keyval_block = gather_directly(keyval_local, ROWS, 1)
    keyval_all = gather_directly(pick_group(keyval_block, head_group), MP, 0)
    scores = jnp.einsum(
        "qhd,kd->hqk", queries, keyval_all[:, :HD], preferred_element_type=jnp.float32
    ) * HD ** (-0.5)
    query_pos = mp_index * share_rows + jnp.arange(share_rows, dtype=jnp.int32)
    key_pos = jnp.arange(total_rows, dtype=jnp.int32)
    allowed = key_pos[None, :] <= query_pos[:, None]
    scores = jnp.where(allowed[None, :, :], scores, -1e30)
    largest = jnp.max(scores, axis=2, keepdims=True)
    powers = jnp.exp(scores - largest)
    probs = (powers / jnp.sum(powers, axis=2, keepdims=True)).astype(jnp.bfloat16)
    context = jnp.einsum(
        "hqk,kd->qhd", probs, keyval_all[:, HD:], preferred_element_type=jnp.float32
    )
    context = context.astype(jnp.bfloat16).reshape(share_rows, query_width)
    context_all = gather_directly(context, MP, 0)
    picked = context_all
    residual = hidden + sent_and_summed(
        tower_rows(picked, w_out, block_towers(modality)).astype(jnp.bfloat16), ROWS, 0
    )
    return ffn(block_towers(modality), residual, ffn_gain, w_gate, w_up, w_down)


def solution(mesh):
    torus = Mesh(mesh.devices.reshape(NX, NYH, 2, 2, NZ), AXES)
    in_specs = (
        P(ROWS, MP),
        P(),
        P(None, MP),
        P(None, MP),
        P(None, MP, ROWS),
        P(None, MP, ROWS),
        P(None, ROWS, MP),
        P(None, MP, ROWS),
        P(None, MP, ROWS),
        P(None, ROWS, MP),
    )
    out_specs = P(ROWS, MP)
    return jax.shard_map(local, mesh=torus, in_specs=in_specs, out_specs=out_specs, check_vma=False)
```

```python
import jax
import jax.numpy as jnp
from jax import lax
from jax.experimental import pallas as pl
from jax.experimental.pallas import tpu as pltpu
from jax.sharding import Mesh
from jax.sharding import PartitionSpec as P

D = 3584
HD = 128
MODAL_BLOCK = 128
ROWS = ("x", "yh", "c")
MP = ("yl", "z")
AXES = ("x", "yh", "c", "yl", "z")
NX, NYH, NZ = 4, 2, 8
NB = NX * NYH

EPSILON = 1e-06
F32 = jnp.float32
BF16 = jnp.bfloat16


class Place:
    def __init__(self):
        self.at = {a: lax.axis_index(a) for a in AXES}
        self.x, self.h, self.c, self.l, self.z = (self.at[a] for a in AXES)
        self.crossed = (self.c - self.l) * (self.c - self.l)
        xa, xb = self.x // NYH, lax.rem(self.x, NYH)
        self.moved = 1 - (1 - (xa - xb) * (xa - xb)) * (1 - (xb - self.h) * (xb - self.h))

    def id(self, **moved):
        return tuple(moved.get(a, self.at[a]) for a in AXES)

    def cross(self, dx, dh):
        return self.id(
            x=lax.rem(self.x + dx, NX), yh=lax.rem(self.h + dh, NYH), c=self.l, yl=self.c
        )

    def ahead(self, dx, dh):
        return NYH * lax.rem(self.x + dx, NX) + lax.rem(self.h + dh, NYH)

    def behind(self, dx, dh):
        return NYH * lax.rem(self.x - dx + NX, NX) + lax.rem(self.h - dh + NYH, NYH)

    def partner(self):
        return self.id(c=1 - self.c)

    def along(self, k):
        return lax.rem(self.z + k + NZ, NZ)

    def up_y(self):
        return lax.rem(self.h + self.l, NYH), 1 - self.l

    def down_y(self):
        return lax.rem(self.h + 1 - self.l, NYH), 1 - self.l

    def keyval_to(self):
        return NYH * lax.rem(self.x, NYH) + self.h, self.x // NYH

    def keyval_from(self):
        return NYH * self.h + self.x // NYH, lax.rem(self.x, NYH)


OFFSETS = tuple((dx, dh) for dx in (2, 1, 3, 0) for dh in (1, 0))


def sent(src, dst, send, recv, target):
    return pltpu.make_async_remote_copy(
        src_ref=src,
        dst_ref=dst,
        send_sem=send,
        recv_sem=recv,
        device_id=target,
        device_id_type=pl.DeviceIdType.MESH,
    )


def greet(place, peers):
    barrier = pltpu.get_barrier_semaphore()

    def hello(peer):
        pl.semaphore_signal(barrier, 1, device_id=peer, device_id_type=pl.DeviceIdType.MESH)

    count = 0
    for peer in peers + [place.cross(*o) for o in OFFSETS if o != (0, 0)]:
        hello(peer)
        count += 1
    xs, hs = place.keyval_from()
    for k in range(1, NZ):
        hello(place.id(x=xs, yh=hs, z=place.along(k)))
        count += 1
    pl.when(place.c != place.l)(lambda: hello(place.cross(0, 0)))
    pl.when(place.moved != 0)(lambda: hello(place.id(x=xs, yh=hs)))
    pl.semaphore_wait(barrier, count + place.crossed + place.moved)


def gather_rows(place, src, xg, sems):
    send, recv, fsend, frecv = (sems.at[k] for k in range(4))
    own = NYH * place.x + place.h
    for i, (dx, dh) in enumerate(OFFSETS):
        copy = sent(src, xg.at[place.l, own], send.at[i], recv.at[i], place.cross(dx, dh))
        if (dx, dh) != (0, 0):
            copy.start()
        else:
            pl.when(place.c != place.l)(copy.start)

            @pl.when(place.c == place.l)
            def _():
                xg[place.l, own] = src[...]

    order = sorted(range(NB), key=lambda i: (min(OFFSETS[i][0], NX - OFFSETS[i][0]), OFFSETS[i][1]))
    for i in order:
        dx, dh = OFFSETS[i]
        slot = xg.at[place.c, place.behind(dx, dh)]
        arrive = sent(slot, slot, send.at[i], recv.at[i], place.cross(dx, dh))
        if (dx, dh) != (0, 0):
            arrive.wait_recv()
        else:
            pl.when(place.c != place.l)(arrive.wait_recv)
        sent(slot, slot, fsend.at[i], frecv.at[i], place.partner()).start()
    for i in order:
        dx, dh = OFFSETS[i]
        slot = xg.at[1 - place.c, place.behind(dx, dh)]
        sent(slot, slot, fsend.at[i], frecv.at[i], place.partner()).wait_recv()


def gather_rows_end(place, src, xg, sems):
    send, recv, fsend, frecv = (sems.at[k] for k in range(4))
    for i, (dx, dh) in enumerate(OFFSETS):
        copy = sent(src, src, send.at[i], recv.at[i], place.cross(dx, dh))
        if (dx, dh) != (0, 0):
            copy.wait_send()
        else:
            pl.when(place.c != place.l)(copy.wait_send)
        slot = xg.at[place.c, place.behind(dx, dh)]
        sent(slot, slot, fsend.at[i], frecv.at[i], place.partner()).wait_send()


def reduce_rows(place, part, dbuf, rbuf, sems):
    send, recv, fsend, frecv = (sems.at[k] for k in range(4))
    own = NYH * place.x + place.h
    for i, (dx, dh) in enumerate(OFFSETS):
        j = place.ahead(dx, dh)
        sent(
            part.at[1 - place.c, j], dbuf.at[j], fsend.at[i], frecv.at[i], place.partner()
        ).start()
    for i, (dx, dh) in enumerate(OFFSETS):
        j = place.ahead(dx, dh)
        sent(part.at[1 - place.c, j], dbuf.at[j], fsend.at[i], frecv.at[i], place.partner()).wait_recv()
        total = part[place.c, j].astype(F32) + dbuf[j].astype(F32)
        dbuf[j] = total.astype(BF16)
        copy = sent(dbuf.at[j], rbuf.at[i], send.at[i], recv.at[i], place.cross(dx, dh))
        if (dx, dh) != (0, 0):
            copy.start()
        else:
            pl.when(place.c != place.l)(copy.start)

            @pl.when(place.c == place.l)
            def _():
                rbuf[i] = dbuf[own]

    total = None
    order = sorted(range(NB), key=lambda i: (min(OFFSETS[i][0], NX - OFFSETS[i][0]), OFFSETS[i][1]))
    for i in order:
        dx, dh = OFFSETS[i]
        arrive = sent(rbuf.at[i], rbuf.at[i], send.at[i], recv.at[i], place.cross(dx, dh))
        if (dx, dh) != (0, 0):
            arrive.wait_recv()
        else:
            pl.when(place.c != place.l)(arrive.wait_recv)
        term = rbuf[i].astype(F32)
        total = term if total is None else total + term
    for i, (dx, dh) in enumerate(OFFSETS):
        j = place.ahead(dx, dh)
        sent(part.at[1 - place.c, j], dbuf.at[j], fsend.at[i], frecv.at[i], place.partner()).wait_send()
        copy = sent(dbuf.at[j], rbuf.at[i], send.at[i], recv.at[i], place.cross(dx, dh))
        if (dx, dh) != (0, 0):
            copy.wait_send()
        else:
            pl.when(place.c != place.l)(copy.wait_send)
    return total


PARTS = 4


def sum_along_z(place, partial, pbuf, chain, sems):
    part_rows = MODAL_BLOCK // PARTS
    sides = (1, -1)

    def rows(q):
        return pl.ds(q * part_rows, part_rows)

    def hops(side, q):
        long = (q < PARTS // 2) == (side == 0)
        return 4 if long else 3

    def link(side, k, q, src):
        return sent(
            src,
            chain.at[side, k - 1, :, rows(q), :],
            sems.at[0, side, k - 1, q],
            sems.at[1, side, k - 1, q],
            place.id(z=place.along(sides[side])),
        )

    partial(place.along(4))
    for q in range(PARTS):
        for side in range(2):
            if hops(side, q) == 4:
                link(side, 4, q, pbuf.at[place.along(4), :, rows(q), :]).start()
    for k in (3, 2, 1):
        for side in range(2):
            partial(place.along(k * sides[side]))
            if k == 3:
                j = place.along(k * sides[side])
                for q in range(PARTS):
                    if hops(side, q) == 3:
                        link(side, 3, q, pbuf.at[j, :, rows(q), :]).start()
        for q in range(PARTS):
            for side in range(2):
                j = place.along(k * sides[side])
                if hops(side, q) == 3 and k == 3:
                    continue
                slot = chain.at[side, k, :, rows(q), :]
                link(side, k + 1, q, slot).wait_recv()
                chain[side, k, :, rows(q), :] = (
                    chain[side, k, :, rows(q), :].astype(F32) + pbuf[j, :, rows(q), :].astype(F32)
                ).astype(BF16)
                link(side, k, q, slot).start()
    partial(place.z)
    for q in range(PARTS):
        for side in range(2):
            slot = chain.at[side, 0, :, rows(q), :]
            link(side, 1, q, slot).wait_recv()
    for q in range(PARTS):
        for side in range(2):
            for k in range(1, hops(side, q) + 1):
                link(side, k, q, chain.at[side, k - 1, :, rows(q), :]).wait_send()


def spread_along_z(place, blocks, sems, on_arrival):
    half = MODAL_BLOCK // 2
    sides = (1, -1)

    def link(side, k, q, owner):
        rows = blocks.at[owner, pl.ds(q * half, half), :]
        return sent(
            rows, rows, sems.at[0, side, k - 1, q], sems.at[1, side, k - 1, q],
            place.id(z=place.along(sides[side])),
        )

    def used(side, k, q):
        return k < 4 or q == side

    for q in range(2):
        for side in range(2):
            link(side, 1, q, place.z).start()
    on_arrival(place.z)
    for k in (1, 2, 3, 4):
        for q in range(2):
            for side in range(2):
                if used(side, k, q):
                    owner = place.along(-k * sides[side])
                    link(side, k, q, owner).wait_recv()
                    if k < 4 and used(side, k + 1, q):
                        link(side, k + 1, q, owner).start()
        if k < 4:
            for side in range(2):
                on_arrival(place.along(-k * sides[side]))
        else:
            on_arrival(place.along(4))
    for k in (1, 2, 3, 4):
        for q in range(2):
            for side in range(2):
                if used(side, k, q):
                    link(side, k, q, place.along(-(k - 1) * sides[side])).wait_send()


def along_order():
    return (4, 3, 5, 2, 6, 1, 7)


def lhs_t(a, b):
    return lax.dot_general(a, b, (((0,), (0,)), ((), ())), preferred_element_type=F32)


def rhs_t(a, b):
    return lax.dot_general(a, b, (((1,), (1,)), ((), ())), preferred_element_type=F32)


def as_column(row):
    return jnp.transpose(jnp.broadcast_to(row, (MODAL_BLOCK, MODAL_BLOCK)))[:, :1]


def layer_kernel(
    towers, tokens, gains, wq_in, wkv_in, wo_in, wg_in, wu_in, wd_in,
    out,
    xa, gother, gcol, wq, wkv, wo, wg, wu, wd,
    qsend, kvsend, qrecv, kvrecv, ssa, ssar, kvown, kvall, scores, ctxs,
    parta, dbufa, rbufa, resid, src,
    xg, pbuf, chain, ssp, ssr, acts, part, dbuf, rbuf,
    lsem, wsem, ga_sem, q_sem, kv_sem, sa_sem, kz_sem, ky_sem, kr_sem, kd_sem, cx_sem, ra_sem,
    g_sem, c_sem, s_sem, a_sem, r_sem,
):
    place = Place()
    own = place.l
    oth = 1 - place.l
    loads = [
        pltpu.make_async_copy(a, b.at[0], lsem.at[k])
        for k, (a, b) in enumerate(
            ((wq_in, wq), (wkv_in, wkv), (wo_in, wo), (wg_in, wg), (wu_in, wu), (wd_in, wd))
        )
    ]
    for load in loads:
        load.start()
    xd, hd = place.keyval_to()
    xs, hs = place.keyval_from()
    uh, ul = place.up_y()
    dh, dl = place.down_y()
    above = place.id(yh=uh, yl=ul)
    below = place.id(yh=dh, yl=dl)
    twin = place.id(yl=1 - place.l)
    greet(
        place,
        [place.partner(), above, below] + [place.id(z=place.along(k)) for k in range(1, NZ)],
    )

    exchange = []
    for k, (a, b) in enumerate(
        [(gains, gother), (wq_in, wq.at[1]), (wkv_in, wkv.at[1]), (wo_in, wo.at[1])]
        + [(w.at[t], v.at[1, t]) for w, v in ((wg_in, wg), (wu_in, wu), (wd_in, wd)) for t in range(2)]
    ):
        exchange.append(sent(a, b, wsem.at[0, k], wsem.at[1, k], twin))

    for e in exchange[:3]:
        e.start()
    gather_rows(place, tokens, xa, ga_sem)
    exchange[3].start()
    exchange[4].start()

    for e in exchange[:3]:
        e.wait_recv()
    for t in range(2):
        for which in range(2):
            for piece, g in enumerate((gains, gother)):
                row = jnp.broadcast_to(g[which * 2 + t], (MODAL_BLOCK, g.shape[2]))
                gcol[which, piece, t] = jnp.transpose(row)
    for load in loads[:2]:
        load.wait()

    def q_copy(k):
        j = place.along(k)
        return sent(qsend.at[j], qrecv.at[place.z], q_sem.at[0, k], q_sem.at[1, k], place.id(z=j))

    def kv_copy(k):
        j = place.along(k)
        return sent(
            kvsend.at[j], kvrecv.at[place.z], kv_sem.at[0, k], kv_sem.at[1, k],
            place.id(x=xd, yh=hd, z=j),
        )

    def ssa_copy(k):
        j = place.along(k)
        return sent(ssa.at[j], ssar.at[place.z], sa_sem.at[0, k], sa_sem.at[1, k], place.id(z=j))

    def squares_of(x0, x1):
        row = jnp.sum(x0 * x0, axis=0, keepdims=True) + jnp.sum(x1 * x1, axis=0, keepdims=True)
        return jnp.broadcast_to(row, (8, MODAL_BLOCK))

    for k in along_order() + (0,):
        j = place.along(k)
        tower = towers[2 * j + place.l]
        x0 = xa[own, j].astype(F32)
        x1 = xa[oth, j].astype(F32)
        ssa[j] = squares_of(x0, x1)
        n0 = (x0 * gcol[0, 0, tower]).astype(BF16)
        n1 = (x1 * gcol[0, 1, tower]).astype(BF16)
        qsend[j] = (lhs_t(wq[0, tower], n0) + lhs_t(wq[1, tower], n1)).astype(BF16)
        kvsend[j] = (
            jnp.dot(wkv[0, tower], n0, preferred_element_type=F32)
            + jnp.dot(wkv[1, tower], n1, preferred_element_type=F32)
        ).astype(BF16)
        if k:
            kv_copy(k).start()
            q_copy(k).start()
            ssa_copy(k).start()
        else:
            pl.when(place.moved != 0)(kv_copy(0).start)

            @pl.when(place.moved == 0)
            def _():
                kvrecv[place.z] = kvsend[place.z]

    squares = ssa[place.z]
    for k in range(1, NZ):
        slot = ssar.at[place.along(-k)]
        sent(slot, slot, sa_sem.at[0, k], sa_sem.at[1, k], twin).wait_recv()
        squares = squares + ssar[place.along(-k)]
    scale = lax.rsqrt(squares[:1] / D + EPSILON)
    for k in range(NZ):
        slot = kvrecv.at[place.along(-k)]
        wait = sent(slot, slot, kv_sem.at[0, k], kv_sem.at[1, k], twin).wait_recv
        if k:
            wait()
        else:
            pl.when(place.moved != 0)(wait)
    kvown[...] = (jnp.sum(kvrecv[...].astype(F32), axis=0) * scale).astype(BF16)

    kvall[place.h, place.l, place.c, place.z] = kvown[...]

    def kz_copy(k):
        return sent(
            kvown, kvall.at[place.h, place.l, place.c, place.z],
            kz_sem.at[0, k], kz_sem.at[1, k], place.id(z=place.along(k)),
        )

    def ky_copy(side, k, ref):
        return sent(ref, ref, ky_sem.at[0, side, k], ky_sem.at[1, side, k], (above, below)[side])

    def kr_copy(k, ref):
        return sent(ref, ref, kr_sem.at[0, k], kr_sem.at[1, k], (above, below)[k % 2])

    def kd_copy(n, ref):
        return sent(ref, ref, kd_sem.at[0, n], kd_sem.at[1, n], place.partner())

    for k in along_order():
        kz_copy(k).start()
    sources = ((place.h, place.l), (dh, dl), (uh, ul), (1 - place.h, place.l))
    near = (0, 1, 7, 2, 6, 3, 5, 4)

    def piece(n, k):
        h, l = sources[n]
        return kvall.at[h, l, place.c, place.along(-k)]

    for k in near:
        if k:
            sent(piece(0, k), piece(0, k), kz_sem.at[0, k], kz_sem.at[1, k], twin).wait_recv()
        for side in range(2):
            ky_copy(side, k, piece(0, k)).start()
    kd_copy(0, kvall.at[place.h, place.l, place.c]).start()
    qt = qsend[place.z].astype(F32)
    for k in range(1, NZ):
        slot = qrecv.at[place.along(-k)]
        sent(slot, slot, q_sem.at[0, k], q_sem.at[1, k], twin).wait_recv()
        qt = qt + qrecv[place.along(-k)].astype(F32)
    qt = (qt * scale).astype(BF16)
    for k in near:
        ky_copy(0, k, piece(1, k)).wait_recv()
        if k % 2 == 0:
            kr_copy(k, piece(1, k)).start()
        ky_copy(1, k, piece(2, k)).wait_recv()
        if k % 2 == 1:
            kr_copy(k, piece(2, k)).start()
    for n in (1, 2):
        kd_copy(n, kvall.at[sources[n][0], sources[n][1], place.c]).start()
    for k in near:
        kr_copy(k, piece(3, k)).wait_recv()
    kd_copy(3, kvall.at[sources[3][0], sources[3][1], place.c]).start()
    for e in exchange[5:8]:
        e.start()
    for n in range(4):
        slot = kvall.at[sources[n][0], sources[n][1], 1 - place.c]
        kd_copy(n, slot).wait_recv()

    qblock = 2 * place.z + place.l

    def keyval(kind, l, z):
        return jnp.concatenate((kvall[kind, l, 0, z], kvall[kind, l, 1, z]), axis=0)

    def score(z, largest):
        for l in range(2):
            b = 2 * z + l
            s = lhs_t(keyval(0, l, z), qt) * HD ** (-0.5)
            shape = (MODAL_BLOCK, MODAL_BLOCK)
            key_pos = b * MODAL_BLOCK + lax.broadcasted_iota(jnp.int32, shape, 0)
            query_pos = qblock * MODAL_BLOCK + lax.broadcasted_iota(jnp.int32, shape, 1)
            s = jnp.where(key_pos <= query_pos, s, -1e30)
            scores[b] = s
            largest = jnp.maximum(largest, jnp.max(s, axis=0, keepdims=True))
        return largest

    largest = lax.fori_loop(0, NZ, score, jnp.full((1, MODAL_BLOCK), -1e30, F32))

    def power(b, norm):
        p = jnp.exp(scores[b] - largest)
        scores[b] = p
        return norm + jnp.sum(p, axis=0, keepdims=True)

    norm = lax.fori_loop(0, 2 * NZ, power, jnp.zeros((1, MODAL_BLOCK), F32))
    inverse = 1.0 / norm

    def weigh(z, ctx):
        for l in range(2):
            p = (scores[2 * z + l] * inverse).astype(BF16)
            ctx = ctx + jnp.dot(keyval(1, l, z), p, preferred_element_type=F32)
        return ctx

    ctxs[place.z] = lax.fori_loop(
        0, NZ, weigh, jnp.zeros((HD, MODAL_BLOCK), F32)
    ).astype(BF16)

    def cx_copy(k, owner):
        return sent(
            ctxs.at[owner], ctxs.at[owner], cx_sem.at[0, k], cx_sem.at[1, k],
            place.id(z=place.along(k)),
        )

    for k in along_order():
        cx_copy(k, place.z).start()
    loads[2].wait()
    exchange[3].wait_recv()
    for k in near:
        j = place.along(-k)
        if k:
            cx_copy(k, j).wait_recv()
        tower = towers[2 * j + place.l]
        parta[own, j] = jnp.dot(wo[0, tower], ctxs[j], preferred_element_type=F32).astype(BF16)
        parta[oth, j] = jnp.dot(wo[1, tower], ctxs[j], preferred_element_type=F32).astype(BF16)
    resid[...] = tokens[...].astype(F32) + reduce_rows(place, parta, dbufa, rbufa, ra_sem)

    src[...] = resid[...].astype(BF16)
    gather_rows(place, src, xg, g_sem)
    for load in loads[3:5]:
        load.wait()
    for e in exchange[4:8]:
        e.wait_recv()
    for e in exchange[8:]:
        e.start()

    def squares_to(k):
        j = place.along(k)
        return sent(ssp.at[j], ssr.at[place.z], s_sem.at[0, k], s_sem.at[1, k], place.id(z=j))

    def partial(j):
        tower = towers[2 * j + place.l]
        x0 = xg[own, j].astype(F32)
        x1 = xg[oth, j].astype(F32)
        ssp[j] = squares_of(x0, x1)
        n0 = (x0 * gcol[1, 0, tower]).astype(BF16)
        n1 = (x1 * gcol[1, 1, tower]).astype(BF16)
        for side, w in enumerate((wg, wu)):
            pbuf[j, side] = (lhs_t(n0, w[0, tower]) + lhs_t(n1, w[1, tower])).astype(BF16)

    sum_along_z(place, partial, pbuf, chain, c_sem)
    for k in range(1, NZ):
        squares_to(k).start()
    both = pbuf[place.z].astype(F32) + chain[0, 0].astype(F32) + chain[1, 0].astype(F32)
    squares = ssp[place.z]
    for k in range(1, NZ):
        slot = ssr.at[place.along(-k)]
        sent(slot, slot, s_sem.at[0, k], s_sem.at[1, k], twin).wait_recv()
        squares = squares + ssr[place.along(-k)]
    scale = as_column(lax.rsqrt(squares[:1] / D + EPSILON))
    gate = both[0] * scale
    up = both[1] * scale
    acts[place.z] = (gate / (1.0 + jnp.exp(-gate)) * up).astype(BF16)
    loads[5].wait()
    for e in exchange[8:]:
        e.wait_recv()

    def downward(j):
        tower = towers[2 * j + place.l]
        act = acts[j]
        part[own, j] = rhs_t(wd[0, tower], act).astype(BF16)
        part[oth, j] = rhs_t(wd[1, tower], act).astype(BF16)

    spread_along_z(place, acts, a_sem, downward)
    total = reduce_rows(place, part, dbuf, rbuf, r_sem)
    out[...] = (resid[...] + total).astype(BF16)

    gather_rows_end(place, tokens, xa, ga_sem)
    gather_rows_end(place, src, xg, g_sem)
    for e in exchange:
        e.wait_send()
    for k in range(1, NZ):
        squares_to(k).wait_send()
        q_copy(k).wait_send()
        kv_copy(k).wait_send()
        ssa_copy(k).wait_send()
        kz_copy(k).wait_send()
        cx_copy(k, place.z).wait_send()
    pl.when(place.moved != 0)(kv_copy(0).wait_send)
    for k in range(NZ):
        for side in range(2):
            ky_copy(side, k, piece(0, k)).wait_send()
        kr_copy(k, piece(1 + k % 2, k)).wait_send()
    for n in range(4):
        kd_copy(n, kvall.at[sources[n][0], sources[n][1], place.c]).wait_send()


def local(tokens, modality, attn_gain, ffn_gain, w_query, w_keyval, w_out, w_gate, w_up, w_down):
    feats = tokens.shape[1]
    width = w_gate.shape[2]
    kvw = w_keyval.shape[2]
    towers = modality.reshape(-1, MODAL_BLOCK)[:, 0]
    gains = jnp.concatenate((attn_gain, ffn_gain), axis=0)[:, None, :]
    vmem = pl.BlockSpec(memory_space=pltpu.VMEM)
    hbm = pl.BlockSpec(memory_space=pltpu.HBM)
    smem = pl.BlockSpec(memory_space=pltpu.SMEM)
    dma = pltpu.SemaphoreType.DMA
    rows = (feats, MODAL_BLOCK)
    result = pl.pallas_call(
        layer_kernel,
        out_shape=jax.ShapeDtypeStruct(rows, BF16),
        in_specs=[smem, vmem, vmem] + [hbm] * 6,
        out_specs=vmem,
        scratch_shapes=[
            pltpu.VMEM((2, NB, *rows), BF16),
            pltpu.VMEM((4, 1, feats), F32),
            pltpu.VMEM((2, 2, 2, *rows), F32),
            pltpu.VMEM((2, 2, feats, HD), BF16),
            pltpu.VMEM((2, 2, kvw, feats), BF16),
            pltpu.VMEM((2, 2, feats, HD), BF16),
            pltpu.VMEM((2, 2, feats, width), BF16),
            pltpu.VMEM((2, 2, feats, width), BF16),
            pltpu.VMEM((2, 2, feats, width), BF16),
            pltpu.VMEM((NZ, HD, MODAL_BLOCK), BF16),
            pltpu.VMEM((NZ, kvw, MODAL_BLOCK), BF16),
            pltpu.VMEM((NZ, HD, MODAL_BLOCK), BF16),
            pltpu.VMEM((NZ, kvw, MODAL_BLOCK), BF16),
            pltpu.VMEM((NZ, 8, MODAL_BLOCK), F32),
            pltpu.VMEM((NZ, 8, MODAL_BLOCK), F32),
            pltpu.VMEM((kvw, MODAL_BLOCK), BF16),
            pltpu.VMEM((2, 2, 2, NZ, kvw, MODAL_BLOCK), BF16),
            pltpu.VMEM((2 * NZ, MODAL_BLOCK, MODAL_BLOCK), F32),
            pltpu.VMEM((NZ, HD, MODAL_BLOCK), BF16),
            pltpu.VMEM((2, NB, *rows), BF16),
            pltpu.VMEM((NB, *rows), BF16),
            pltpu.VMEM((NB, *rows), BF16),
            pltpu.VMEM(rows, F32),
            pltpu.VMEM(rows, BF16),
            pltpu.VMEM((2, NB, *rows), BF16),
            pltpu.VMEM((NZ, 2, MODAL_BLOCK, width), BF16),
            pltpu.VMEM((2, 4, 2, MODAL_BLOCK, width), BF16),
            pltpu.VMEM((NZ, 8, MODAL_BLOCK), F32),
            pltpu.VMEM((NZ, 8, MODAL_BLOCK), F32),
            pltpu.VMEM((NZ, MODAL_BLOCK, width), BF16),
            pltpu.VMEM((2, NB, *rows), BF16),
            pltpu.VMEM((NB, *rows), BF16),
            pltpu.VMEM((NB, *rows), BF16),
            dma((6,)),
            dma((2, 10)),
            dma((4, NB)),
            dma((2, NZ)),
            dma((2, NZ)),
            dma((2, NZ)),
            dma((2, NZ)),
            dma((2, 2, NZ)),
            dma((2, NZ)),
            dma((2, 4)),
            dma((2, NZ)),
            dma((4, NB)),
            dma((4, NB)),
            dma((2, 2, 4, PARTS)),
            dma((2, NZ)),
            dma((2, 2, 4, 2)),
            dma((4, NB)),
        ],
        compiler_params=pltpu.CompilerParams(collective_id=0, has_side_effects=True),
        name="layer",
    )(
        towers,
        tokens.T,
        gains,
        w_query,
        jnp.swapaxes(w_keyval, 1, 2),
        jnp.swapaxes(w_out, 1, 2),
        w_gate,
        w_up,
        jnp.swapaxes(w_down, 1, 2),
    )
    return result.T


def solution(mesh):
    torus = Mesh(mesh.devices.reshape(NX, NYH, 2, 2, NZ), AXES)
    in_specs = (
        P(ROWS, MP),
        P(),
        P(None, MP),
        P(None, MP),
        P(None, MP, ROWS),
        P(None, MP, ROWS),
        P(None, ROWS, MP),
        P(None, MP, ROWS),
        P(None, MP, ROWS),
        P(None, ROWS, MP),
    )
    out_specs = P(ROWS, MP)
    return jax.shard_map(local, mesh=torus, in_specs=in_specs, out_specs=out_specs, check_vma=False)
```

```python
import jax
import jax.numpy as jnp
from jax import lax
from jax.experimental import pallas as pl
from jax.experimental.pallas import tpu as pltpu
from jax.sharding import Mesh
from jax.sharding import PartitionSpec as P

D = 3584
HD = 128
MODAL_BLOCK = 128
ROWS = ("x", "yh", "c")
MP = ("yl", "z")
AXES = ("x", "yh", "c", "yl", "z")
NX, NYH, NZ = 4, 2, 8
NB = NX * NYH

EPSILON = 1e-06
F32 = jnp.float32
BF16 = jnp.bfloat16


class Place:
    def __init__(self):
        self.at = {a: lax.axis_index(a) for a in AXES}
        self.x, self.h, self.c, self.l, self.z = (self.at[a] for a in AXES)
        self.crossed = (self.c - self.l) * (self.c - self.l)
        xa, xb = self.x // NYH, lax.rem(self.x, NYH)
        self.moved = 1 - (1 - (xa - xb) * (xa - xb)) * (1 - (xb - self.h) * (xb - self.h))

    def id(self, **moved):
        return tuple(moved.get(a, self.at[a]) for a in AXES)

    def cross(self, dx, dh):
        return self.id(
            x=lax.rem(self.x + dx, NX), yh=lax.rem(self.h + dh, NYH), c=self.l, yl=self.c
        )

    def ahead(self, dx, dh):
        return NYH * lax.rem(self.x + dx, NX) + lax.rem(self.h + dh, NYH)

    def behind(self, dx, dh):
        return NYH * lax.rem(self.x - dx + NX, NX) + lax.rem(self.h - dh + NYH, NYH)

    def partner(self):
        return self.id(c=1 - self.c)

    def along(self, k):
        return lax.rem(self.z + k + NZ, NZ)

    def up_y(self):
        return lax.rem(self.h + self.l, NYH), 1 - self.l

    def down_y(self):
        return lax.rem(self.h + 1 - self.l, NYH), 1 - self.l

    def keyval_to(self):
        return NYH * lax.rem(self.x, NYH) + self.h, self.x // NYH

    def keyval_from(self):
        return NYH * self.h + self.x // NYH, lax.rem(self.x, NYH)


OFFSETS = tuple((dx, dh) for dx in (2, 1, 3, 0) for dh in (1, 0))


def sent(src, dst, send, recv, target):
    return pltpu.make_async_remote_copy(
        src_ref=src,
        dst_ref=dst,
        send_sem=send,
        recv_sem=recv,
        device_id=target,
        device_id_type=pl.DeviceIdType.MESH,
    )


def greet(place, peers):
    barrier = pltpu.get_barrier_semaphore()

    def hello(peer):
        pl.semaphore_signal(barrier, 1, device_id=peer, device_id_type=pl.DeviceIdType.MESH)

    count = 0
    for peer in peers + [place.cross(*o) for o in OFFSETS if o != (0, 0)]:
        hello(peer)
        count += 1
    xs, hs = place.keyval_from()
    for k in range(1, NZ):
        hello(place.id(x=xs, yh=hs, z=place.along(k)))
        count += 1
    pl.when(place.c != place.l)(lambda: hello(place.cross(0, 0)))
    pl.when(place.moved != 0)(lambda: hello(place.id(x=xs, yh=hs)))
    pl.semaphore_wait(barrier, count + place.crossed + place.moved)


def arrivals(place):
    order = sorted(OFFSETS, key=lambda o: (min(o[0], NX - o[0]), o[1]))
    return [place.behind(*o) for o in order]


class RowGather:
    def __init__(self, place, src, xg, sems):
        self.place, self.src, self.xg = place, src, xg
        self.send, self.recv, self.fsend, self.frecv = (sems.at[k] for k in range(4))
        self.own = NYH * place.x + place.h

    def away(self, j):
        return jnp.logical_or(j != self.own, self.place.c != self.place.l)

    def copy(self, i):
        return sent(
            self.src,
            self.xg.at[self.place.l, self.own],
            self.send.at[i],
            self.recv.at[self.own],
            self.place.cross(*OFFSETS[i]),
        )

    def start(self):
        place = self.place
        for i, offset in enumerate(OFFSETS):
            if offset != (0, 0):
                self.copy(i).start()
            else:
                pl.when(place.c != place.l)(self.copy(i).start)

                @pl.when(place.c == place.l)
                def _():
                    self.xg[place.l, self.own] = self.src[...]

    def forwarding(self, j, piece):
        slot = self.xg.at[piece, j]
        return sent(slot, slot, self.fsend.at[j], self.frecv.at[j], self.place.partner())

    def forward(self, j):
        slot = self.xg.at[self.place.c, j]
        arrive = sent(slot, slot, self.send.at[0], self.recv.at[j], self.place.partner())
        pl.when(self.away(j))(arrive.wait_recv)
        self.forwarding(j, self.place.c).start()

    def ready(self, j):
        self.forwarding(j, 1 - self.place.c).wait_recv()

    def end(self):
        for i, offset in enumerate(OFFSETS):
            if offset != (0, 0):
                self.copy(i).wait_send()
            else:
                pl.when(self.place.c != self.place.l)(self.copy(i).wait_send)
        for j in range(NB):
            self.forwarding(j, self.place.c).wait_send()


class RowSum:
    def __init__(self, place, part, dbuf, rbuf, sems):
        self.place, self.part, self.dbuf, self.rbuf = place, part, dbuf, rbuf
        self.send, self.recv, self.fsend, self.frecv = (sems.at[k] for k in range(4))
        self.own = NYH * place.x + place.h

    def away(self, j):
        return jnp.logical_or(j != self.own, self.place.c != self.place.l)

    def pairing(self, j):
        return sent(
            self.part.at[1 - self.place.c, j],
            self.dbuf.at[j],
            self.fsend.at[j],
            self.frecv.at[j],
            self.place.partner(),
        )

    def copy(self, j):
        return sent(
            self.dbuf.at[j],
            self.rbuf.at[self.own],
            self.send.at[j],
            self.recv.at[self.own],
            self.place.id(x=j // NYH, yh=lax.rem(j, NYH), c=self.place.l, yl=self.place.c),
        )

    def pair(self, j):
        self.pairing(j).start()

    def pass_on(self, j):
        self.pairing(j).wait_recv()
        total = self.part[self.place.c, j].astype(F32) + self.dbuf[j].astype(F32)
        self.dbuf[j] = total.astype(BF16)
        pl.when(self.away(j))(self.copy(j).start)

        @pl.when(jnp.logical_not(self.away(j)))
        def _():
            self.rbuf[self.own] = self.dbuf[self.own]

    def finish(self):
        total = None
        for j in arrivals(self.place):
            slot = self.rbuf.at[j]
            arrive = sent(slot, slot, self.send.at[0], self.recv.at[j], self.place.partner())
            pl.when(self.away(j))(arrive.wait_recv)
            term = self.rbuf[j].astype(F32)
            total = term if total is None else total + term
        return total

    def end(self):
        for j in range(NB):
            self.pairing(j).wait_send()
            pl.when(self.away(j))(self.copy(j).wait_send)


PARTS = 4
LOOK = 3
LAG = 2


def sum_along_z(place, partial, pbuf, chain, sems):
    part_rows = MODAL_BLOCK // PARTS
    sides = (1, -1)

    def rows(q):
        return pl.ds(q * part_rows, part_rows)

    def hops(side, q):
        long = (q < PARTS // 2) == (side == 0)
        return 4 if long else 3

    def link(side, k, q, src):
        return sent(
            src,
            chain.at[side, k - 1, :, rows(q), :],
            sems.at[0, side, k - 1, q],
            sems.at[1, side, k - 1, q],
            place.id(z=place.along(sides[side])),
        )

    partial(place.along(4))
    for q in range(PARTS):
        for side in range(2):
            if hops(side, q) == 4:
                link(side, 4, q, pbuf.at[place.along(4), :, rows(q), :]).start()
    for k in (3, 2, 1):
        for side in range(2):
            partial(place.along(k * sides[side]))
            if k == 3:
                j = place.along(k * sides[side])
                for q in range(PARTS):
                    if hops(side, q) == 3:
                        link(side, 3, q, pbuf.at[j, :, rows(q), :]).start()
        for q in range(PARTS):
            for side in range(2):
                j = place.along(k * sides[side])
                if hops(side, q) == 3 and k == 3:
                    continue
                slot = chain.at[side, k, :, rows(q), :]
                link(side, k + 1, q, slot).wait_recv()
                chain[side, k, :, rows(q), :] = (
                    chain[side, k, :, rows(q), :].astype(F32) + pbuf[j, :, rows(q), :].astype(F32)
                ).astype(BF16)
                link(side, k, q, slot).start()
    partial(place.z)
    for q in range(PARTS):
        for side in range(2):
            slot = chain.at[side, 0, :, rows(q), :]
            link(side, 1, q, slot).wait_recv()
    for q in range(PARTS):
        for side in range(2):
            for k in range(1, hops(side, q) + 1):
                link(side, k, q, chain.at[side, k - 1, :, rows(q), :]).wait_send()


def spread_along_z(place, blocks, sems, on_arrival):
    part_rows = MODAL_BLOCK // PARTS
    sides = (1, -1)

    def link(side, k, q, owner):
        rows = blocks.at[owner, pl.ds(q * part_rows, part_rows), :]
        return sent(
            rows, rows, sems.at[0, side, k - 1, q], sems.at[1, side, k - 1, q],
            place.id(z=place.along(sides[side])),
        )

    def used(side, k, q):
        return k < 4 or (q < PARTS // 2) == (side == 0)

    for q in range(PARTS):
        for side in range(2):
            link(side, 1, q, place.z).start()
    on_arrival(place.z)
    for k in (1, 2, 3, 4):
        for q in range(PARTS):
            for side in range(2):
                if used(side, k, q):
                    owner = place.along(-k * sides[side])
                    link(side, k, q, owner).wait_recv()
                    if k < 4 and used(side, k + 1, q):
                        link(side, k + 1, q, owner).start()
        if k < 4:
            for side in range(2):
                on_arrival(place.along(-k * sides[side]))
        else:
            on_arrival(place.along(4))
    for k in (1, 2, 3, 4):
        for q in range(PARTS):
            for side in range(2):
                if used(side, k, q):
                    link(side, k, q, place.along(-(k - 1) * sides[side])).wait_send()


def along_order():
    return (4, 3, 5, 2, 6, 1, 7)


def lhs_t(a, b):
    return lax.dot_general(a, b, (((0,), (0,)), ((), ())), preferred_element_type=F32)


def rhs_t(a, b):
    return lax.dot_general(a, b, (((1,), (1,)), ((), ())), preferred_element_type=F32)


def as_column(row):
    return jnp.transpose(jnp.broadcast_to(row, (MODAL_BLOCK, MODAL_BLOCK)))[:, :1]


def layer_kernel(
    modality, tokens, again, fgain, wq_in, wkv_in, wo_in, wg_in, wu_in, wd_in,
    out,
    xa, gother, fother, gcol, wq, wkv, wo, wg, wu, wd,
    qsend, kvsend, qrecv, kvrecv, ssa, ssar, kvown, kvall, scores, ctxs,
    parta, dbufa, rbufa, resid, src,
    xg, pbuf, chain, ssp, ssr, acts, part, dbuf, rbuf,
    lsem, wsem, ga_sem, q_sem, kv_sem, sa_sem, kz_sem, ky_sem, kr_sem, kd_sem, cx_sem, ra_sem,
    g_sem, c_sem, s_sem, a_sem, r_sem,
):
    place = Place()
    own = place.l
    oth = 1 - place.l
    loads = [
        pltpu.make_async_copy(a, b.at[0], lsem.at[k])
        for k, (a, b) in enumerate(
            ((wq_in, wq), (wkv_in, wkv), (wo_in, wo), (wg_in, wg), (wu_in, wu), (wd_in, wd))
        )
    ]
    for load in loads:
        load.start()
    xd, hd = place.keyval_to()
    xs, hs = place.keyval_from()
    uh, ul = place.up_y()
    dh, dl = place.down_y()
    above = place.id(yh=uh, yl=ul)
    below = place.id(yh=dh, yl=dl)
    twin = place.id(yl=1 - place.l)
    greet(
        place,
        [place.partner(), above, below] + [place.id(z=place.along(k)) for k in range(1, NZ)],
    )

    exchange = []
    for k, (a, b) in enumerate(
        [(again, gother), (wq_in, wq.at[1]), (wkv_in, wkv.at[1]), (wo_in, wo.at[1])]
        + [(w.at[t], v.at[1, t]) for w, v in ((wg_in, wg), (wu_in, wu), (wd_in, wd)) for t in range(2)]
        + [(fgain, fother)]
    ):
        exchange.append(sent(a, b, wsem.at[0, k], wsem.at[1, k], twin))

    rows_in = RowGather(place, tokens, xa, ga_sem)
    for e in exchange[:3] + exchange[10:]:
        e.start()
    rows_in.start()

    def tower_of(j):
        return modality[MODAL_BLOCK * (2 * j + place.l)]

    exchange[0].wait_recv()
    exchange[10].wait_recv()
    for t in range(2):
        for which, pair in enumerate(((again, gother), (fgain, fother))):
            for piece, g in enumerate(pair):
                row = jnp.broadcast_to(g[t : t + 1, :], (MODAL_BLOCK, g.shape[1]))
                gcol[which, piece, t] = jnp.transpose(row)
    for load in loads[:2]:
        load.wait()
    coming = arrivals(place)
    for e in exchange[1:3]:
        e.wait_recv()
    for j in coming[:LOOK]:
        rows_in.forward(j)

    def q_copy(j):
        return sent(
            qsend.at[j], qrecv.at[place.z], q_sem.at[0, j], q_sem.at[1, place.z], place.id(z=j)
        )

    def kv_copy(j):
        return sent(
            kvsend.at[j], kvrecv.at[place.z], kv_sem.at[0, j], kv_sem.at[1, place.z],
            place.id(x=xd, yh=hd, z=j),
        )

    def ssa_copy(j):
        return sent(
            ssa.at[j], ssar.at[place.z], sa_sem.at[0, j], sa_sem.at[1, place.z], place.id(z=j)
        )

    def stays(j):
        return jnp.logical_and(j == place.z, place.moved == 0)

    def send_block(j):
        pl.when(jnp.logical_not(stays(j)))(lambda: kv_copy(j).start())

        @pl.when(stays(j))
        def _():
            kvrecv[place.z] = kvsend[place.z]

        @pl.when(j != place.z)
        def _():
            q_copy(j).start()
            ssa_copy(j).start()

    def squares_of(x0, x1):
        row = jnp.sum(x0 * x0, axis=0, keepdims=True) + jnp.sum(x1 * x1, axis=0, keepdims=True)
        return jnp.broadcast_to(row, (8, MODAL_BLOCK))

    for n, j in enumerate(coming):
        if n + LOOK < NB:
            rows_in.forward(coming[n + LOOK])
        rows_in.ready(j)
        tower = tower_of(j)
        x0 = xa[own, j].astype(F32)
        x1 = xa[oth, j].astype(F32)
        ssa[j] = squares_of(x0, x1)
        n0 = (x0 * gcol[0, 0, tower]).astype(BF16)
        n1 = (x1 * gcol[0, 1, tower]).astype(BF16)
        qsend[j] = (lhs_t(wq[0, tower], n0) + lhs_t(wq[1, tower], n1)).astype(BF16)
        kvsend[j] = (
            jnp.dot(wkv[0, tower], n0, preferred_element_type=F32)
            + jnp.dot(wkv[1, tower], n1, preferred_element_type=F32)
        ).astype(BF16)
        send_block(j)

    for e in exchange[3:6]:
        e.start()
    squares = ssa[place.z]
    for k in range(1, NZ):
        slot = ssar.at[place.along(-k)]
        sent(slot, slot, sa_sem.at[0, k], sa_sem.at[1, place.along(-k)], twin).wait_recv()
        squares = squares + ssar[place.along(-k)]
    scale = lax.rsqrt(squares[:1] / D + EPSILON)
    for k in range(NZ):
        slot = kvrecv.at[place.along(-k)]
        wait = sent(slot, slot, kv_sem.at[0, k], kv_sem.at[1, place.along(-k)], twin).wait_recv
        if k:
            wait()
        else:
            pl.when(place.moved != 0)(wait)
    kvown[...] = (jnp.sum(kvrecv[...].astype(F32), axis=0) * scale).astype(BF16)

    kvall[place.h, place.l, place.c, place.z] = kvown[...]

    def kz_copy(k):
        return sent(
            kvown, kvall.at[place.h, place.l, place.c, place.z],
            kz_sem.at[0, k], kz_sem.at[1, k], place.id(z=place.along(k)),
        )

    def ky_copy(side, k, ref):
        return sent(ref, ref, ky_sem.at[0, side, k], ky_sem.at[1, side, k], (above, below)[side])

    def kr_copy(k, ref):
        return sent(ref, ref, kr_sem.at[0, k], kr_sem.at[1, k], (above, below)[k % 2])

    def kd_copy(n, ref):
        return sent(ref, ref, kd_sem.at[0, n], kd_sem.at[1, n], place.partner())

    for k in along_order():
        kz_copy(k).start()
    sources = ((place.h, place.l), (dh, dl), (uh, ul), (1 - place.h, place.l))
    near = (0, 1, 7, 2, 6, 3, 5, 4)

    def piece(n, k):
        h, l = sources[n]
        return kvall.at[h, l, place.c, place.along(-k)]

    for k in near:
        if k:
            sent(piece(0, k), piece(0, k), kz_sem.at[0, k], kz_sem.at[1, k], twin).wait_recv()
        for side in range(2):
            ky_copy(side, k, piece(0, k)).start()
    kd_copy(0, kvall.at[place.h, place.l, place.c]).start()
    qt = qsend[place.z].astype(F32)
    for k in range(1, NZ):
        slot = qrecv.at[place.along(-k)]
        sent(slot, slot, q_sem.at[0, k], q_sem.at[1, place.along(-k)], twin).wait_recv()
        qt = qt + qrecv[place.along(-k)].astype(F32)
    qt = (qt * scale).astype(BF16)
    for k in near:
        ky_copy(0, k, piece(1, k)).wait_recv()
        if k % 2 == 0:
            kr_copy(k, piece(1, k)).start()
        ky_copy(1, k, piece(2, k)).wait_recv()
        if k % 2 == 1:
            kr_copy(k, piece(2, k)).start()
    for n in (1, 2):
        kd_copy(n, kvall.at[sources[n][0], sources[n][1], place.c]).start()
    for k in near:
        kr_copy(k, piece(3, k)).wait_recv()
    kd_copy(3, kvall.at[sources[3][0], sources[3][1], place.c]).start()
    for e in exchange[6:8]:
        e.start()
    for n in range(4):
        slot = kvall.at[sources[n][0], sources[n][1], 1 - place.c]
        kd_copy(n, slot).wait_recv()

    qblock = 2 * place.z + place.l

    def keyval(kind, l, z):
        return jnp.concatenate((kvall[kind, l, 0, z], kvall[kind, l, 1, z]), axis=0)

    def score(z, largest):
        for l in range(2):
            b = 2 * z + l
            s = lhs_t(keyval(0, l, z), qt) * HD ** (-0.5)
            shape = (MODAL_BLOCK, MODAL_BLOCK)
            key_pos = b * MODAL_BLOCK + lax.broadcasted_iota(jnp.int32, shape, 0)
            query_pos = qblock * MODAL_BLOCK + lax.broadcasted_iota(jnp.int32, shape, 1)
            s = jnp.where(key_pos <= query_pos, s, -1e30)
            scores[b] = s
            largest = jnp.maximum(largest, jnp.max(s, axis=0, keepdims=True))
        return largest

    largest = lax.fori_loop(0, NZ, score, jnp.full((1, MODAL_BLOCK), -1e30, F32))

    def power(b, norm):
        p = jnp.exp(scores[b] - largest)
        scores[b] = p
        return norm + jnp.sum(p, axis=0, keepdims=True)

    norm = lax.fori_loop(0, 2 * NZ, power, jnp.zeros((1, MODAL_BLOCK), F32))
    inverse = 1.0 / norm

    def weigh(z, ctx):
        for l in range(2):
            p = (scores[2 * z + l] * inverse).astype(BF16)
            ctx = ctx + jnp.dot(keyval(1, l, z), p, preferred_element_type=F32)
        return ctx

    ctxs[place.z] = lax.fori_loop(
        0, NZ, weigh, jnp.zeros((HD, MODAL_BLOCK), F32)
    ).astype(BF16)

    def cx(k, owner):
        first = 64 if k == -4 else 0
        ref = ctxs.at[owner, pl.ds(first, HD // 2 if abs(k) == 4 else HD), :]
        n = 0 if k == -4 else k % NZ
        step = {3: 1, -3: -1, 4: 2, -4: -2}.get(k, k)
        return sent(ref, ref, cx_sem.at[0, n], cx_sem.at[1, n], place.id(z=place.along(step)))

    for k in (2, -2, 1, -1):
        cx(k, place.z).start()
    loads[2].wait()
    exchange[3].wait_recv()
    rows_out = RowSum(place, parta, dbufa, rbufa, ra_sem)

    def outward(j):
        tower = tower_of(j)
        parta[own, j] = jnp.dot(wo[0, tower], ctxs[j], preferred_element_type=F32).astype(BF16)
        parta[oth, j] = jnp.dot(wo[1, tower], ctxs[j], preferred_element_type=F32).astype(BF16)
        rows_out.pair(j)

    outward(place.z)
    for side in (1, -1):
        owner = place.along(-2 * side)
        cx(2 * side, owner).wait_recv()
        cx(3 * side, owner).start()
        cx(4 * side, owner).start()
    last = place.z
    for k in (1, -1, 2, -2, 3, -3, 4):
        j = place.along(-k)
        if abs(k) != 2:
            cx(k, j).wait_recv()
        if k == 4:
            cx(-4, j).wait_recv()
        outward(j)
        rows_out.pass_on(last)
        last = j
    rows_out.pass_on(last)
    resid[...] = tokens[...].astype(F32) + rows_out.finish()

    src[...] = resid[...].astype(BF16)
    rows_mid = RowGather(place, src, xg, g_sem)
    rows_mid.start()
    needed = [place.along(k) for k in (4, 3, -3, 2, -2, 1, -1, 0)]
    for j in needed[:LOOK]:
        rows_mid.forward(j)
    for load in loads[3:5]:
        load.wait()
    for e in exchange[4:8]:
        e.wait_recv()
    for e in exchange[8:10]:
        e.start()

    def squares_to(k):
        j = place.along(k)
        return sent(ssp.at[j], ssr.at[place.z], s_sem.at[0, k], s_sem.at[1, k], place.id(z=j))

    called = []

    def partial(j):
        n = len(called)
        called.append(j)
        if n + LOOK < NB:
            rows_mid.forward(needed[n + LOOK])
        rows_mid.ready(needed[n])
        tower = tower_of(j)
        x0 = xg[own, j].astype(F32)
        x1 = xg[oth, j].astype(F32)
        ssp[j] = squares_of(x0, x1)
        n0 = (x0 * gcol[1, 0, tower]).astype(BF16)
        n1 = (x1 * gcol[1, 1, tower]).astype(BF16)
        for side, w in enumerate((wg, wu)):
            pbuf[j, side] = (lhs_t(n0, w[0, tower]) + lhs_t(n1, w[1, tower])).astype(BF16)
        if n + 1 < NB:
            squares_to((4, 3, -3, 2, -2, 1, -1)[n] % NZ).start()

    sum_along_z(place, partial, pbuf, chain, c_sem)
    both = pbuf[place.z].astype(F32) + chain[0, 0].astype(F32) + chain[1, 0].astype(F32)
    squares = ssp[place.z]
    for k in range(1, NZ):
        slot = ssr.at[place.along(-k)]
        sent(slot, slot, s_sem.at[0, k], s_sem.at[1, k], twin).wait_recv()
        squares = squares + ssr[place.along(-k)]
    scale = as_column(lax.rsqrt(squares[:1] / D + EPSILON))
    gate = both[0] * scale
    up = both[1] * scale
    acts[place.z] = (gate / (1.0 + jnp.exp(-gate)) * up).astype(BF16)
    loads[5].wait()
    for e in exchange[8:10]:
        e.wait_recv()

    rows_end = RowSum(place, part, dbuf, rbuf, r_sem)
    done = []

    def downward(j):
        tower = tower_of(j)
        act = acts[j]
        part[own, j] = rhs_t(wd[0, tower], act).astype(BF16)
        part[oth, j] = rhs_t(wd[1, tower], act).astype(BF16)
        rows_end.pair(j)
        if len(done) >= LAG:
            rows_end.pass_on(done[-LAG])
        done.append(j)

    spread_along_z(place, acts, a_sem, downward)
    for j in done[-LAG:]:
        rows_end.pass_on(j)
    total = rows_end.finish()
    out[...] = (resid[...] + total).astype(BF16)

    rows_in.end()
    rows_mid.end()
    rows_out.end()
    rows_end.end()
    for e in exchange:
        e.wait_send()
    for k in range(1, NZ):
        j = place.along(k)
        squares_to(k).wait_send()
        q_copy(j).wait_send()
        kv_copy(j).wait_send()
        ssa_copy(j).wait_send()
        kz_copy(k).wait_send()
    for side in (1, -1):
        for k in (1, 2):
            cx(k * side, place.z).wait_send()
        for k in (3, 4):
            cx(k * side, place.along(-2 * side)).wait_send()
    pl.when(place.moved != 0)(kv_copy(place.z).wait_send)
    for k in range(NZ):
        for side in range(2):
            ky_copy(side, k, piece(0, k)).wait_send()
        kr_copy(k, piece(1 + k % 2, k)).wait_send()
    for n in range(4):
        kd_copy(n, kvall.at[sources[n][0], sources[n][1], place.c]).wait_send()


def local(tokens, modality, attn_gain, ffn_gain, w_query, w_keyval, w_out, w_gate, w_up, w_down):
    feats = tokens.shape[1]
    width = w_gate.shape[2]
    kvw = w_keyval.shape[2]
    vmem = pl.BlockSpec(memory_space=pltpu.VMEM)
    hbm = pl.BlockSpec(memory_space=pltpu.HBM)
    smem = pl.BlockSpec(memory_space=pltpu.SMEM)
    dma = pltpu.SemaphoreType.DMA
    rows = (feats, MODAL_BLOCK)
    result = pl.pallas_call(
        layer_kernel,
        out_shape=jax.ShapeDtypeStruct(rows, BF16),
        in_specs=[smem, vmem, vmem, vmem] + [hbm] * 6,
        out_specs=vmem,
        scratch_shapes=[
            pltpu.VMEM((2, NB, *rows), BF16),
            pltpu.VMEM((2, feats), F32),
            pltpu.VMEM((2, feats), F32),
            pltpu.VMEM((2, 2, 2, *rows), F32),
            pltpu.VMEM((2, 2, feats, HD), BF16),
            pltpu.VMEM((2, 2, kvw, feats), BF16),
            pltpu.VMEM((2, 2, feats, HD), BF16),
            pltpu.VMEM((2, 2, feats, width), BF16),
            pltpu.VMEM((2, 2, feats, width), BF16),
            pltpu.VMEM((2, 2, feats, width), BF16),
            pltpu.VMEM((NZ, HD, MODAL_BLOCK), BF16),
            pltpu.VMEM((NZ, kvw, MODAL_BLOCK), BF16),
            pltpu.VMEM((NZ, HD, MODAL_BLOCK), BF16),
            pltpu.VMEM((NZ, kvw, MODAL_BLOCK), BF16),
            pltpu.VMEM((NZ, 8, MODAL_BLOCK), F32),
            pltpu.VMEM((NZ, 8, MODAL_BLOCK), F32),
            pltpu.VMEM((kvw, MODAL_BLOCK), BF16),
            pltpu.VMEM((2, 2, 2, NZ, kvw, MODAL_BLOCK), BF16),
            pltpu.VMEM((2 * NZ, MODAL_BLOCK, MODAL_BLOCK), F32),
            pltpu.VMEM((NZ, HD, MODAL_BLOCK), BF16),
            pltpu.VMEM((2, NB, *rows), BF16),
            pltpu.VMEM((NB, *rows), BF16),
            pltpu.VMEM((NB, *rows), BF16),
            pltpu.VMEM(rows, F32),
            pltpu.VMEM(rows, BF16),
            pltpu.VMEM((2, NB, *rows), BF16),
            pltpu.VMEM((NZ, 2, MODAL_BLOCK, width), BF16),
            pltpu.VMEM((2, 4, 2, MODAL_BLOCK, width), BF16),
            pltpu.VMEM((NZ, 8, MODAL_BLOCK), F32),
            pltpu.VMEM((NZ, 8, MODAL_BLOCK), F32),
            pltpu.VMEM((NZ, MODAL_BLOCK, width), BF16),
            pltpu.VMEM((2, NB, *rows), BF16),
            pltpu.VMEM((NB, *rows), BF16),
            pltpu.VMEM((NB, *rows), BF16),
            dma((6,)),
            dma((2, 11)),
            dma((4, NB)),
            dma((2, NZ)),
            dma((2, NZ)),
            dma((2, NZ)),
            dma((2, NZ)),
            dma((2, 2, NZ)),
            dma((2, NZ)),
            dma((2, 4)),
            dma((2, NZ)),
            dma((4, NB)),
            dma((4, NB)),
            dma((2, 2, 4, PARTS)),
            dma((2, NZ)),
            dma((2, 2, 4, PARTS)),
            dma((4, NB)),
        ],
        compiler_params=pltpu.CompilerParams(collective_id=0, has_side_effects=True),
        name="layer",
    )(
        modality,
        tokens.T,
        attn_gain,
        ffn_gain,
        w_query,
        jnp.swapaxes(w_keyval, 1, 2),
        jnp.swapaxes(w_out, 1, 2),
        w_gate,
        w_up,
        jnp.swapaxes(w_down, 1, 2),
    )
    return result.T


def solution(mesh):
    torus = Mesh(mesh.devices.reshape(NX, NYH, 2, 2, NZ), AXES)
    in_specs = (
        P(ROWS, MP),
        P(),
        P(None, MP),
        P(None, MP),
        P(None, MP, ROWS),
        P(None, MP, ROWS),
        P(None, ROWS, MP),
        P(None, MP, ROWS),
        P(None, MP, ROWS),
        P(None, ROWS, MP),
    )
    out_specs = P(ROWS, MP)
    return jax.shard_map(local, mesh=torus, in_specs=in_specs, out_specs=out_specs, check_vma=False)
```

```python
import jax
import jax.numpy as jnp
from jax import lax
from jax.experimental import pallas as pl
from jax.experimental.pallas import tpu as pltpu
from jax.sharding import Mesh
from jax.sharding import PartitionSpec as P

D = 3584
HD = 128
MODAL_BLOCK = 128
ROWS = ("x", "yh", "c")
MP = ("yl", "z")
AXES = ("x", "yh", "c", "yl", "z")
NX, NYH, NZ = 4, 2, 8
NB = NX * NYH

EPSILON = 1e-06
F32 = jnp.float32
BF16 = jnp.bfloat16


class Place:
    def __init__(self):
        self.at = {a: lax.axis_index(a) for a in AXES}
        self.x, self.h, self.c, self.l, self.z = (self.at[a] for a in AXES)
        self.crossed = (self.c - self.l) * (self.c - self.l)
        xa, xb = self.x // NYH, lax.rem(self.x, NYH)
        self.moved = 1 - (1 - (xa - xb) * (xa - xb)) * (1 - (xb - self.h) * (xb - self.h))

    def id(self, **moved):
        return tuple(moved.get(a, self.at[a]) for a in AXES)

    def cross(self, dx, dh):
        return self.id(
            x=lax.rem(self.x + dx, NX), yh=lax.rem(self.h + dh, NYH), c=self.l, yl=self.c
        )

    def ahead(self, dx, dh):
        return NYH * lax.rem(self.x + dx, NX) + lax.rem(self.h + dh, NYH)

    def behind(self, dx, dh):
        return NYH * lax.rem(self.x - dx + NX, NX) + lax.rem(self.h - dh + NYH, NYH)

    def partner(self):
        return self.id(c=1 - self.c)

    def along(self, k):
        return lax.rem(self.z + k + NZ, NZ)

    def up_y(self):
        return lax.rem(self.h + self.l, NYH), 1 - self.l

    def down_y(self):
        return lax.rem(self.h + 1 - self.l, NYH), 1 - self.l

    def keyval_to(self):
        return NYH * lax.rem(self.x, NYH) + self.h, self.x // NYH

    def keyval_from(self):
        return NYH * self.h + self.x // NYH, lax.rem(self.x, NYH)


OFFSETS = tuple((dx, dh) for dx in (2, 1, 3, 0) for dh in (1, 0))


def sent(src, dst, send, recv, target):
    return pltpu.make_async_remote_copy(
        src_ref=src,
        dst_ref=dst,
        send_sem=send,
        recv_sem=recv,
        device_id=target,
        device_id_type=pl.DeviceIdType.MESH,
    )


def greet(place, peers):
    barrier = pltpu.get_barrier_semaphore()

    def hello(peer):
        pl.semaphore_signal(barrier, 1, device_id=peer, device_id_type=pl.DeviceIdType.MESH)

    count = 0
    for peer in peers + [place.cross(*o) for o in OFFSETS if o != (0, 0)]:
        hello(peer)
        count += 1
    xs, hs = place.keyval_from()
    for k in range(1, NZ):
        hello(place.id(x=xs, yh=hs, z=place.along(k)))
        count += 1
    pl.when(place.c != place.l)(lambda: hello(place.cross(0, 0)))
    pl.when(place.moved != 0)(lambda: hello(place.id(x=xs, yh=hs)))
    pl.semaphore_wait(barrier, count + place.crossed + place.moved)


def arrivals(place):
    order = sorted(OFFSETS, key=lambda o: (min(o[0], NX - o[0]), o[1]))
    return [place.behind(*o) for o in order]


class RowGather:
    def __init__(self, place, src, xg, sems):
        self.place, self.src, self.xg = place, src, xg
        self.send, self.recv, self.fsend, self.frecv = (sems.at[k] for k in range(4))
        self.own = NYH * place.x + place.h

    def away(self, j):
        return jnp.logical_or(j != self.own, self.place.c != self.place.l)

    def copy(self, i):
        return sent(
            self.src,
            self.xg.at[self.place.l, self.own],
            self.send.at[i],
            self.recv.at[self.own],
            self.place.cross(*OFFSETS[i]),
        )

    def start(self):
        place = self.place
        for i, offset in enumerate(OFFSETS):
            if offset != (0, 0):
                self.copy(i).start()
            else:
                pl.when(place.c != place.l)(self.copy(i).start)

                @pl.when(place.c == place.l)
                def _():
                    self.xg[place.l, self.own] = self.src[...]

    def forwarding(self, j, piece):
        slot = self.xg.at[piece, j]
        return sent(slot, slot, self.fsend.at[j], self.frecv.at[j], self.place.partner())

    def forward(self, j):
        slot = self.xg.at[self.place.c, j]
        arrive = sent(slot, slot, self.send.at[0], self.recv.at[j], self.place.partner())
        pl.when(self.away(j))(arrive.wait_recv)
        self.forwarding(j, self.place.c).start()

    def ready(self, j):
        self.forwarding(j, 1 - self.place.c).wait_recv()

    def end(self):
        for i, offset in enumerate(OFFSETS):
            if offset != (0, 0):
                self.copy(i).wait_send()
            else:
                pl.when(self.place.c != self.place.l)(self.copy(i).wait_send)
        for j in range(NB):
            self.forwarding(j, self.place.c).wait_send()


class RowSum:
    def __init__(self, place, part, dbuf, rbuf, sems):
        self.place, self.part, self.dbuf, self.rbuf = place, part, dbuf, rbuf
        self.send, self.recv, self.fsend, self.frecv = (sems.at[k] for k in range(4))
        self.own = NYH * place.x + place.h

    def away(self, j):
        return jnp.logical_or(j != self.own, self.place.c != self.place.l)

    def pairing(self, j):
        return sent(
            self.part.at[1 - self.place.c, j],
            self.dbuf.at[j],
            self.fsend.at[j],
            self.frecv.at[j],
            self.place.partner(),
        )

    def copy(self, j):
        return sent(
            self.dbuf.at[j],
            self.rbuf.at[self.own],
            self.send.at[j],
            self.recv.at[self.own],
            self.place.id(x=j // NYH, yh=lax.rem(j, NYH), c=self.place.l, yl=self.place.c),
        )

    def pair(self, j):
        self.pairing(j).start()

    def pass_on(self, j):
        self.pairing(j).wait_recv()
        total = self.part[self.place.c, j].astype(F32) + self.dbuf[j].astype(F32)
        self.dbuf[j] = total.astype(BF16)
        pl.when(self.away(j))(self.copy(j).start)

        @pl.when(jnp.logical_not(self.away(j)))
        def _():
            self.rbuf[self.own] = self.dbuf[self.own]

    def finish(self):
        total = None
        for j in arrivals(self.place):
            slot = self.rbuf.at[j]
            arrive = sent(slot, slot, self.send.at[0], self.recv.at[j], self.place.partner())
            pl.when(self.away(j))(arrive.wait_recv)
            term = self.rbuf[j].astype(F32)
            total = term if total is None else total + term
        return total

    def end(self):
        for j in range(NB):
            self.pairing(j).wait_send()
            pl.when(self.away(j))(self.copy(j).wait_send)


PARTS = 4


def part_of(width, q):
    tiles = width // 16
    starts = [16 * (tiles * p // PARTS) for p in range(PARTS)] + [width]
    return pl.ds(starts[q], starts[q + 1] - starts[q])


LOOK = 3
LAG = 2


def sum_along_z(place, partial, pbuf, chain, sems, on_part):
    sides = (1, -1)

    def rows(q):
        return part_of(pbuf.shape[2], q)

    def hops(side, q):
        long = (q < PARTS // 2) == (side == 0)
        return 4 if long else 3

    def link(side, k, q, src):
        return sent(
            src,
            chain.at[side, k - 1, :, rows(q), :],
            sems.at[0, side, k - 1, q],
            sems.at[1, side, k - 1, q],
            place.id(z=place.along(sides[side])),
        )

    partial(place.along(4))
    for q in range(PARTS):
        for side in range(2):
            if hops(side, q) == 4:
                link(side, 4, q, pbuf.at[place.along(4), :, rows(q), :]).start()
    for k in (3, 2, 1):
        for side in range(2):
            partial(place.along(k * sides[side]))
            if k == 3:
                j = place.along(k * sides[side])
                for q in range(PARTS):
                    if hops(side, q) == 3:
                        link(side, 3, q, pbuf.at[j, :, rows(q), :]).start()
        for q in range(PARTS):
            for side in range(2):
                j = place.along(k * sides[side])
                if hops(side, q) == 3 and k == 3:
                    continue
                slot = chain.at[side, k, :, rows(q), :]
                link(side, k + 1, q, slot).wait_recv()
                chain[side, k, :, rows(q), :] = (
                    chain[side, k, :, rows(q), :].astype(F32) + pbuf[j, :, rows(q), :].astype(F32)
                ).astype(BF16)
                link(side, k, q, slot).start()
    partial(place.z)
    for q in range(PARTS):
        for side in range(2):
            slot = chain.at[side, 0, :, rows(q), :]
            link(side, 1, q, slot).wait_recv()
        on_part(q, rows(q))
    for q in range(PARTS):
        for side in range(2):
            for k in range(1, hops(side, q) + 1):
                link(side, k, q, chain.at[side, k - 1, :, rows(q), :]).wait_send()


class Ring:
    def __init__(self, place, blocks, sems):
        self.place, self.blocks, self.sems = place, blocks, sems
        self.all = [(q, side) for q in range(PARTS) for side in range(2)]

    def link(self, side, k, q, owner):
        rows = self.blocks.at[owner, part_of(self.blocks.shape[1], q), :]
        step = (1, -1)[side]
        return sent(
            rows,
            rows,
            self.sems.at[0, side, k - 1, q],
            self.sems.at[1, side, k - 1, q],
            self.place.id(z=self.place.along(step)),
        )

    def used(self, side, k, q):
        return k < 4 or (q < PARTS // 2) == (side == 0)

    def start(self, q):
        for side in range(2):
            self.link(side, 1, q, self.place.z).start()

    def run(self, on_arrival):
        on_arrival(self.place.z)
        for k in (1, 2, 3, 4):
            for q, side in self.all:
                if self.used(side, k, q):
                    owner = self.place.along((-k, k)[side])
                    self.link(side, k, q, owner).wait_recv()
                    if k < 4 and self.used(side, k + 1, q):
                        self.link(side, k + 1, q, owner).start()
            on_arrival(self.place.along(-k))
            if k < 4:
                on_arrival(self.place.along(k))

    def end(self):
        for k in (1, 2, 3, 4):
            for q, side in self.all:
                if self.used(side, k, q):
                    self.link(side, k, q, self.place.along((1 - k, k - 1)[side])).wait_send()


def along_order():
    return (4, 3, 5, 2, 6, 1, 7)


def lhs_t(a, b):
    return lax.dot_general(a, b, (((0,), (0,)), ((), ())), preferred_element_type=F32)


def rhs_t(a, b):
    return lax.dot_general(a, b, (((1,), (1,)), ((), ())), preferred_element_type=F32)


def layer_kernel(
    modality, tokens, again, fgain, wq_in, wkv_in, wo_in, wg_in, wu_in, wd_in,
    out,
    xa, gother, fother, gcol, wq, wkv, wo, wg, wu, wd,
    turned, qsend, kvsend, qrecv, kvrecv, ssa, ssar, kvown, kvall, scores, ctxs,
    parta, dbufa, rbufa, resid, src,
    xg, pbuf, chain, ssp, ssr, acts, part, dbuf, rbuf,
    lsem, wsem, ga_sem, q_sem, kv_sem, sa_sem, kz_sem, ky_sem, kr_sem, kd_sem, cx_sem, ra_sem,
    g_sem, c_sem, s_sem, a_sem, r_sem,
):
    place = Place()
    own = place.l
    oth = 1 - place.l
    loads = [
        pltpu.make_async_copy(a, b.at[0], lsem.at[k])
        for k, (a, b) in enumerate(
            ((wq_in, wq), (wkv_in, wkv), (wo_in, wo), (wg_in, wg), (wu_in, wu), (wd_in, wd))
        )
    ]
    for load in loads:
        load.start()
    xd, hd = place.keyval_to()
    xs, hs = place.keyval_from()
    uh, ul = place.up_y()
    dh, dl = place.down_y()
    above = place.id(yh=uh, yl=ul)
    below = place.id(yh=dh, yl=dl)
    twin = place.id(yl=1 - place.l)
    greet(
        place,
        [place.partner(), above, below] + [place.id(z=place.along(k)) for k in range(1, NZ)],
    )

    exchange = []
    for k, (a, b) in enumerate(
        [(again, gother), (wq_in, wq.at[1]), (wkv_in, wkv.at[1]), (wo_in, wo.at[1])]
        + [(w.at[t], v.at[1, t]) for w, v in ((wg_in, wg), (wu_in, wu), (wd_in, wd)) for t in range(2)]
        + [(fgain, fother)]
    ):
        exchange.append(sent(a, b, wsem.at[0, k], wsem.at[1, k], twin))

    rows_in = RowGather(place, tokens, xa, ga_sem)
    for e in exchange[:3] + exchange[10:]:
        e.start()
    rows_in.start()

    def tower_of(j):
        return modality[MODAL_BLOCK * (2 * j + place.l)]

    exchange[0].wait_recv()
    exchange[10].wait_recv()
    for t in range(2):
        for which, pair in enumerate(((again, gother), (fgain, fother))):
            for piece, g in enumerate(pair):
                row = jnp.broadcast_to(g[t : t + 1, :], (MODAL_BLOCK, g.shape[1]))
                gcol[which, piece, t] = jnp.transpose(row)
    for load in loads[:2]:
        load.wait()
    coming = arrivals(place)
    for e in exchange[1:3]:
        e.wait_recv()
    for j in coming[:LOOK]:
        rows_in.forward(j)

    def q_copy(j):
        return sent(
            qsend.at[j], qrecv.at[place.z], q_sem.at[0, j], q_sem.at[1, place.z], place.id(z=j)
        )

    def kv_copy(j):
        return sent(
            kvsend.at[j], kvrecv.at[place.z], kv_sem.at[0, j], kv_sem.at[1, place.z],
            place.id(x=xd, yh=hd, z=j),
        )

    def ssa_copy(j):
        return sent(
            ssa.at[j], ssar.at[place.z], sa_sem.at[0, j], sa_sem.at[1, place.z], place.id(z=j)
        )

    def stays(j):
        return jnp.logical_and(j == place.z, place.moved == 0)

    def send_block(j):
        pl.when(jnp.logical_not(stays(j)))(lambda: kv_copy(j).start())

        @pl.when(stays(j))
        def _():
            kvrecv[place.z] = kvsend[place.z]

        @pl.when(j != place.z)
        def _():
            q_copy(j).start()
            ssa_copy(j).start()

    def squares_of(x0, x1):
        row = jnp.sum(x0 * x0, axis=0, keepdims=True) + jnp.sum(x1 * x1, axis=0, keepdims=True)
        return jnp.broadcast_to(row, (8, MODAL_BLOCK))

    for n, j in enumerate(coming):
        if n + LOOK < NB:
            rows_in.forward(coming[n + LOOK])
        rows_in.ready(j)
        tower = tower_of(j)
        x0 = xa[own, j].astype(F32)
        x1 = xa[oth, j].astype(F32)
        ssa[j] = squares_of(x0, x1)
        n0 = (x0 * gcol[0, 0, tower]).astype(BF16)
        n1 = (x1 * gcol[0, 1, tower]).astype(BF16)
        qsend[j] = (lhs_t(wq[0, tower], n0) + lhs_t(wq[1, tower], n1)).astype(BF16)
        kvsend[j] = (
            jnp.dot(wkv[0, tower], n0, preferred_element_type=F32)
            + jnp.dot(wkv[1, tower], n1, preferred_element_type=F32)
        ).astype(BF16)
        send_block(j)

    for e in exchange[3:6]:
        e.start()
    def turn(side, piece):
        for t in range(2):
            turned[side, piece, t] = jnp.transpose(
                (wg, wu)[side][piece, t].astype(F32)
            ).astype(BF16)

    for side in range(2):
        loads[3 + side].wait()
        turn(side, 0)
    squares = ssa[place.z]
    for k in range(1, NZ):
        slot = ssar.at[place.along(-k)]
        sent(slot, slot, sa_sem.at[0, k], sa_sem.at[1, place.along(-k)], twin).wait_recv()
        squares = squares + ssar[place.along(-k)]
    scale = lax.rsqrt(squares[:1] / D + EPSILON)
    for k in range(NZ):
        slot = kvrecv.at[place.along(-k)]
        wait = sent(slot, slot, kv_sem.at[0, k], kv_sem.at[1, place.along(-k)], twin).wait_recv
        if k:
            wait()
        else:
            pl.when(place.moved != 0)(wait)
    kvown[...] = (jnp.sum(kvrecv[...].astype(F32), axis=0) * scale).astype(BF16)

    kvall[place.h, place.l, place.c, place.z] = kvown[...]

    def kz_copy(k):
        return sent(
            kvown, kvall.at[place.h, place.l, place.c, place.z],
            kz_sem.at[0, k], kz_sem.at[1, k], place.id(z=place.along(k)),
        )

    def ky_copy(side, k, ref):
        return sent(ref, ref, ky_sem.at[0, side, k], ky_sem.at[1, side, k], (above, below)[side])

    def kr_copy(k, ref):
        return sent(ref, ref, kr_sem.at[0, k], kr_sem.at[1, k], (above, below)[k % 2])

    def kd_copy(n, ref):
        return sent(ref, ref, kd_sem.at[0, n], kd_sem.at[1, n], place.partner())

    for k in along_order():
        kz_copy(k).start()
    sources = ((place.h, place.l), (dh, dl), (uh, ul), (1 - place.h, place.l))
    near = (0, 1, 7, 2, 6, 3, 5, 4)

    def piece(n, k):
        h, l = sources[n]
        return kvall.at[h, l, place.c, place.along(-k)]

    for k in near:
        if k:
            sent(piece(0, k), piece(0, k), kz_sem.at[0, k], kz_sem.at[1, k], twin).wait_recv()
        for side in range(2):
            ky_copy(side, k, piece(0, k)).start()
    kd_copy(0, kvall.at[place.h, place.l, place.c]).start()
    qt = qsend[place.z].astype(F32)
    for k in range(1, NZ):
        slot = qrecv.at[place.along(-k)]
        sent(slot, slot, q_sem.at[0, k], q_sem.at[1, place.along(-k)], twin).wait_recv()
        qt = qt + qrecv[place.along(-k)].astype(F32)
    qt = qt * scale
    qt = qt.astype(BF16).astype(F32)
    for k in near:
        ky_copy(0, k, piece(1, k)).wait_recv()
        if k % 2 == 0:
            kr_copy(k, piece(1, k)).start()
        ky_copy(1, k, piece(2, k)).wait_recv()
        if k % 2 == 1:
            kr_copy(k, piece(2, k)).start()
    for n in (1, 2):
        kd_copy(n, kvall.at[sources[n][0], sources[n][1], place.c]).start()
    for k in near:
        kr_copy(k, piece(3, k)).wait_recv()
    kd_copy(3, kvall.at[sources[3][0], sources[3][1], place.c]).start()
    for e in exchange[6:8]:
        e.start()
    for n in range(4):
        slot = kvall.at[sources[n][0], sources[n][1], 1 - place.c]
        kd_copy(n, slot).wait_recv()

    qblock = 2 * place.z + place.l

    def keyval(kind, l, z):
        return jnp.concatenate((kvall[kind, l, 0, z], kvall[kind, l, 1, z]), axis=0)

    shape = (MODAL_BLOCK, MODAL_BLOCK)
    query = jnp.transpose(qt).astype(BF16)
    ahead = lax.broadcasted_iota(jnp.int32, shape, 1) - lax.broadcasted_iota(jnp.int32, shape, 0)
    largest = jnp.full(shape, -1e30, F32)
    for z in range(NZ):
        for l in range(2):
            b = 2 * z + l
            s = jnp.dot(query, keyval(0, l, z), preferred_element_type=F32) * HD ** (-0.5)
            s = jnp.where(ahead <= (qblock - b) * MODAL_BLOCK, s, -1e30)
            scores[b] = s
            largest = jnp.maximum(largest, s)
    largest = jnp.max(largest, axis=1, keepdims=True)
    norm = jnp.zeros(shape, F32)
    for b in range(2 * NZ):
        p = jnp.exp(scores[b] - largest)
        scores[b] = p
        norm = norm + p
    inverse = 1.0 / jnp.sum(norm, axis=1, keepdims=True)
    ctx = jnp.zeros((MODAL_BLOCK, HD), F32)
    for z in range(NZ):
        for l in range(2):
            p = (scores[2 * z + l] * inverse).astype(BF16)
            ctx = ctx + rhs_t(p, keyval(1, l, z))
    ctxs[place.z] = jnp.transpose(ctx).astype(BF16)

    def cx(k, owner):
        first = 64 if k == -4 else 0
        ref = ctxs.at[owner, pl.ds(first, HD // 2 if abs(k) == 4 else HD), :]
        n = 0 if k == -4 else k % NZ
        step = {3: 1, -3: -1, 4: 2, -4: -2}.get(k, k)
        return sent(ref, ref, cx_sem.at[0, n], cx_sem.at[1, n], place.id(z=place.along(step)))

    for k in (2, -2, 1, -1):
        cx(k, place.z).start()
    for e in exchange[4:6]:
        e.wait_recv()
    turn(0, 1)
    loads[2].wait()
    exchange[3].wait_recv()
    rows_out = RowSum(place, parta, dbufa, rbufa, ra_sem)

    def outward(j):
        tower = tower_of(j)
        parta[own, j] = jnp.dot(wo[0, tower], ctxs[j], preferred_element_type=F32).astype(BF16)
        parta[oth, j] = jnp.dot(wo[1, tower], ctxs[j], preferred_element_type=F32).astype(BF16)
        rows_out.pair(j)

    outward(place.z)
    for side in (1, -1):
        owner = place.along(-2 * side)
        cx(2 * side, owner).wait_recv()
        cx(3 * side, owner).start()
        cx(4 * side, owner).start()
    sums = [place.z]
    for k in (1, -1, 2, -2, 3, -3, 4):
        j = place.along(-k)
        if abs(k) != 2:
            cx(k, j).wait_recv()
        if k == 4:
            cx(-4, j).wait_recv()
        outward(j)
        if len(sums) >= LAG:
            rows_out.pass_on(sums[-LAG])
        sums.append(j)
    for j in sums[-LAG:]:
        rows_out.pass_on(j)
    resid[...] = tokens[...].astype(F32) + rows_out.finish()

    src[...] = resid[...].astype(BF16)
    rows_mid = RowGather(place, src, xg, g_sem)
    rows_mid.start()
    for e in exchange[6:8]:
        e.wait_recv()
    turn(1, 1)
    needed = [place.along(k) for k in (4, 3, -3, 2, -2, 1, -1, 0)]
    for j in needed[:LOOK]:
        rows_mid.forward(j)
    for e in exchange[8:10]:
        e.start()

    def squares_to(k):
        j = place.along(k)
        return sent(ssp.at[j], ssr.at[place.z], s_sem.at[0, k], s_sem.at[1, k], place.id(z=j))

    called = []

    def partial(j):
        n = len(called)
        called.append(j)
        if n + LOOK < NB:
            rows_mid.forward(needed[n + LOOK])
        rows_mid.ready(needed[n])
        tower = tower_of(j)
        x0 = xg[own, j].astype(F32)
        x1 = xg[oth, j].astype(F32)
        ssp[j] = squares_of(x0, x1)
        n0 = (x0 * gcol[1, 0, tower]).astype(BF16)
        n1 = (x1 * gcol[1, 1, tower]).astype(BF16)
        for side in range(2):
            pbuf[j, side] = (
                jnp.dot(turned[side, 0, tower], n0, preferred_element_type=F32)
                + jnp.dot(turned[side, 1, tower], n1, preferred_element_type=F32)
            ).astype(BF16)
        if n + 1 < NB:
            squares_to((4, 3, -3, 2, -2, 1, -1)[n] % NZ).start()

    ring = Ring(place, acts, a_sem)
    scales = []

    def activate(q, rows):
        if not scales:
            squares = ssp[place.z]
            for k in range(1, NZ):
                slot = ssr.at[place.along(-k)]
                sent(slot, slot, s_sem.at[0, k], s_sem.at[1, k], twin).wait_recv()
                squares = squares + ssr[place.along(-k)]
            scales.append(lax.rsqrt(squares[:1] / D + EPSILON))
        gate, up = (
            (
                pbuf[place.z, side, rows, :].astype(F32)
                + chain[0, 0, side, rows, :].astype(F32)
                + chain[1, 0, side, rows, :].astype(F32)
            )
            * scales[0]
            for side in range(2)
        )
        acts[place.z, rows, :] = (gate / (1.0 + jnp.exp(-gate)) * up).astype(BF16)
        ring.start(q)

    sum_along_z(place, partial, pbuf, chain, c_sem, activate)
    loads[5].wait()
    for e in exchange[8:10]:
        e.wait_recv()
    rows_end = RowSum(place, part, dbuf, rbuf, r_sem)
    done = []

    def downward(j):
        tower = tower_of(j)
        act = acts[j]
        part[own, j] = jnp.dot(wd[0, tower], act, preferred_element_type=F32).astype(BF16)
        part[oth, j] = jnp.dot(wd[1, tower], act, preferred_element_type=F32).astype(BF16)
        rows_end.pair(j)
        if len(done) >= LAG:
            rows_end.pass_on(done[-LAG])
        done.append(j)

    ring.run(downward)
    for j in done[-LAG:]:
        rows_end.pass_on(j)
    total = rows_end.finish()
    out[...] = (resid[...] + total).astype(BF16)

    ring.end()
    rows_in.end()
    rows_mid.end()
    rows_out.end()
    rows_end.end()
    for e in exchange:
        e.wait_send()
    for k in range(1, NZ):
        j = place.along(k)
        squares_to(k).wait_send()
        q_copy(j).wait_send()
        kv_copy(j).wait_send()
        ssa_copy(j).wait_send()
        kz_copy(k).wait_send()
    for side in (1, -1):
        for k in (1, 2):
            cx(k * side, place.z).wait_send()
        for k in (3, 4):
            cx(k * side, place.along(-2 * side)).wait_send()
    pl.when(place.moved != 0)(kv_copy(place.z).wait_send)
    for k in range(NZ):
        for side in range(2):
            ky_copy(side, k, piece(0, k)).wait_send()
        kr_copy(k, piece(1 + k % 2, k)).wait_send()
    for n in range(4):
        kd_copy(n, kvall.at[sources[n][0], sources[n][1], place.c]).wait_send()


def local(tokens, modality, attn_gain, ffn_gain, w_query, w_keyval, w_out, w_gate, w_up, w_down):
    feats = tokens.shape[1]
    width = w_gate.shape[2]
    kvw = w_keyval.shape[2]
    vmem = pl.BlockSpec(memory_space=pltpu.VMEM)
    hbm = pl.BlockSpec(memory_space=pltpu.HBM)
    smem = pl.BlockSpec(memory_space=pltpu.SMEM)
    dma = pltpu.SemaphoreType.DMA
    rows = (feats, MODAL_BLOCK)
    result = pl.pallas_call(
        layer_kernel,
        out_shape=jax.ShapeDtypeStruct(rows, BF16),
        in_specs=[smem, vmem, vmem, vmem] + [hbm] * 6,
        out_specs=vmem,
        scratch_shapes=[
            pltpu.VMEM((2, NB, *rows), BF16),
            pltpu.VMEM((2, feats), F32),
            pltpu.VMEM((2, feats), F32),
            pltpu.VMEM((2, 2, 2, *rows), F32),
            pltpu.VMEM((2, 2, feats, HD), BF16),
            pltpu.VMEM((2, 2, kvw, feats), BF16),
            pltpu.VMEM((2, 2, feats, HD), BF16),
            pltpu.VMEM((2, 2, feats, width), BF16),
            pltpu.VMEM((2, 2, feats, width), BF16),
            pltpu.VMEM((2, 2, feats, width), BF16),
            pltpu.VMEM((2, 2, 2, width, feats), BF16),
            pltpu.VMEM((NZ, HD, MODAL_BLOCK), BF16),
            pltpu.VMEM((NZ, kvw, MODAL_BLOCK), BF16),
            pltpu.VMEM((NZ, HD, MODAL_BLOCK), BF16),
            pltpu.VMEM((NZ, kvw, MODAL_BLOCK), BF16),
            pltpu.VMEM((NZ, 8, MODAL_BLOCK), F32),
            pltpu.VMEM((NZ, 8, MODAL_BLOCK), F32),
            pltpu.VMEM((kvw, MODAL_BLOCK), BF16),
            pltpu.VMEM((2, 2, 2, NZ, kvw, MODAL_BLOCK), BF16),
            pltpu.VMEM((2 * NZ, MODAL_BLOCK, MODAL_BLOCK), F32),
            pltpu.VMEM((NZ, HD, MODAL_BLOCK), BF16),
            pltpu.VMEM((2, NB, *rows), BF16),
            pltpu.VMEM((NB, *rows), BF16),
            pltpu.VMEM((NB, *rows), BF16),
            pltpu.VMEM(rows, F32),
            pltpu.VMEM(rows, BF16),
            pltpu.VMEM((2, NB, *rows), BF16),
            pltpu.VMEM((NZ, 2, width, MODAL_BLOCK), BF16),
            pltpu.VMEM((2, 4, 2, width, MODAL_BLOCK), BF16),
            pltpu.VMEM((NZ, 8, MODAL_BLOCK), F32),
            pltpu.VMEM((NZ, 8, MODAL_BLOCK), F32),
            pltpu.VMEM((NZ, width, MODAL_BLOCK), BF16),
            pltpu.VMEM((2, NB, *rows), BF16),
            pltpu.VMEM((NB, *rows), BF16),
            pltpu.VMEM((NB, *rows), BF16),
            dma((6,)),
            dma((2, 11)),
            dma((4, NB)),
            dma((2, NZ)),
            dma((2, NZ)),
            dma((2, NZ)),
            dma((2, NZ)),
            dma((2, 2, NZ)),
            dma((2, NZ)),
            dma((2, 4)),
            dma((2, NZ)),
            dma((4, NB)),
            dma((4, NB)),
            dma((2, 2, 4, PARTS)),
            dma((2, NZ)),
            dma((2, 2, 4, PARTS)),
            dma((4, NB)),
        ],
        compiler_params=pltpu.CompilerParams(collective_id=0, has_side_effects=True),
        name="layer",
    )(
        modality,
        tokens.T,
        attn_gain,
        ffn_gain,
        w_query,
        jnp.swapaxes(w_keyval, 1, 2),
        jnp.swapaxes(w_out, 1, 2),
        w_gate,
        w_up,
        jnp.swapaxes(w_down, 1, 2),
    )
    return result.T


def solution(mesh):
    torus = Mesh(mesh.devices.reshape(NX, NYH, 2, 2, NZ), AXES)
    in_specs = (
        P(ROWS, MP),
        P(),
        P(None, MP),
        P(None, MP),
        P(None, MP, ROWS),
        P(None, MP, ROWS),
        P(None, ROWS, MP),
        P(None, MP, ROWS),
        P(None, MP, ROWS),
        P(None, ROWS, MP),
    )
    out_specs = P(ROWS, MP)
    return jax.shard_map(local, mesh=torus, in_specs=in_specs, out_specs=out_specs, check_vma=False)
```

```python
import jax
import jax.numpy as jnp
from jax import lax
from jax.experimental import pallas as pl
from jax.experimental.pallas import tpu as pltpu
from jax.sharding import Mesh
from jax.sharding import PartitionSpec as P

D = 3584
HD = 128
MODAL_BLOCK = 128
ROWS = ("x", "yh", "c")
MP = ("yl", "z")
AXES = ("x", "yh", "c", "yl", "z")
NX, NYH, NZ = 4, 2, 8
NB = NX * NYH

EPSILON = 1e-06
F32 = jnp.float32
BF16 = jnp.bfloat16


class Place:
    def __init__(self):
        self.at = {a: lax.axis_index(a) for a in AXES}
        self.x, self.h, self.c, self.l, self.z = (self.at[a] for a in AXES)
        self.crossed = (self.c - self.l) * (self.c - self.l)
        xa, xb = self.x // NYH, lax.rem(self.x, NYH)
        self.moved = 1 - (1 - (xa - xb) * (xa - xb)) * (1 - (xb - self.h) * (xb - self.h))

    def id(self, **moved):
        return tuple(moved.get(a, self.at[a]) for a in AXES)

    def cross(self, dx, dh):
        return self.id(
            x=lax.rem(self.x + dx, NX), yh=lax.rem(self.h + dh, NYH), c=self.l, yl=self.c
        )

    def ahead(self, dx, dh):
        return NYH * lax.rem(self.x + dx, NX) + lax.rem(self.h + dh, NYH)

    def behind(self, dx, dh):
        return NYH * lax.rem(self.x - dx + NX, NX) + lax.rem(self.h - dh + NYH, NYH)

    def partner(self):
        return self.id(c=1 - self.c)

    def along(self, k):
        return lax.rem(self.z + k + NZ, NZ)

    def up_y(self):
        return lax.rem(self.h + self.l, NYH), 1 - self.l

    def down_y(self):
        return lax.rem(self.h + 1 - self.l, NYH), 1 - self.l

    def keyval_to(self):
        return NYH * lax.rem(self.x, NYH) + self.h, self.x // NYH

    def keyval_from(self):
        return NYH * self.h + self.x // NYH, lax.rem(self.x, NYH)


OFFSETS = tuple((dx, dh) for dx in (2, 1, 3, 0) for dh in (1, 0))


def sent(src, dst, send, recv, target):
    return pltpu.make_async_remote_copy(
        src_ref=src,
        dst_ref=dst,
        send_sem=send,
        recv_sem=recv,
        device_id=target,
        device_id_type=pl.DeviceIdType.MESH,
    )


def greet(place, peers):
    barrier = pltpu.get_barrier_semaphore()

    def hello(peer):
        pl.semaphore_signal(barrier, 1, device_id=peer, device_id_type=pl.DeviceIdType.MESH)

    count = 0
    for peer in peers + [place.cross(*o) for o in OFFSETS if o != (0, 0)]:
        hello(peer)
        count += 1
    xs, hs = place.keyval_from()
    for k in range(1, NZ):
        hello(place.id(x=xs, yh=hs, z=place.along(k)))
        count += 1
    pl.when(place.c != place.l)(lambda: hello(place.cross(0, 0)))
    pl.when(place.moved != 0)(lambda: hello(place.id(x=xs, yh=hs)))
    pl.semaphore_wait(barrier, count + place.crossed + place.moved)


def arrivals(place):
    order = sorted(OFFSETS, key=lambda o: (min(o[0], NX - o[0]), o[1]))
    return [place.behind(*o) for o in order]


class RowGather:
    def __init__(self, place, src, xg, sems):
        self.place, self.src, self.xg = place, src, xg
        self.send, self.recv, self.fsend, self.frecv = (sems.at[k] for k in range(4))
        self.own = NYH * place.x + place.h

    def away(self, j):
        return jnp.logical_or(j != self.own, self.place.c != self.place.l)

    def copy(self, i):
        return sent(
            self.src,
            self.xg.at[self.place.l, self.own],
            self.send.at[i],
            self.recv.at[self.own],
            self.place.cross(*OFFSETS[i]),
        )

    def start(self):
        place = self.place
        for i, offset in enumerate(OFFSETS):
            if offset != (0, 0):
                self.copy(i).start()
            else:
                pl.when(place.c != place.l)(self.copy(i).start)

                @pl.when(place.c == place.l)
                def _():
                    self.xg[place.l, self.own] = self.src[...]

    def forwarding(self, j, piece):
        slot = self.xg.at[piece, j]
        return sent(slot, slot, self.fsend.at[j], self.frecv.at[j], self.place.partner())

    def forward(self, j):
        slot = self.xg.at[self.place.c, j]
        arrive = sent(slot, slot, self.send.at[0], self.recv.at[j], self.place.partner())
        pl.when(self.away(j))(arrive.wait_recv)
        self.forwarding(j, self.place.c).start()

    def ready(self, j):
        self.forwarding(j, 1 - self.place.c).wait_recv()

    def end(self):
        for i, offset in enumerate(OFFSETS):
            if offset != (0, 0):
                self.copy(i).wait_send()
            else:
                pl.when(self.place.c != self.place.l)(self.copy(i).wait_send)
        for j in range(NB):
            self.forwarding(j, self.place.c).wait_send()


class RowSum:
    def __init__(self, place, part, dbuf, rbuf, sems):
        self.place, self.part, self.dbuf, self.rbuf = place, part, dbuf, rbuf
        self.send, self.recv, self.fsend, self.frecv = (sems.at[k] for k in range(4))
        self.own = NYH * place.x + place.h

    def away(self, j):
        return jnp.logical_or(j != self.own, self.place.c != self.place.l)

    def pairing(self, j):
        return sent(
            self.part.at[1 - self.place.c, j],
            self.dbuf.at[j],
            self.fsend.at[j],
            self.frecv.at[j],
            self.place.partner(),
        )

    def copy(self, j):
        return sent(
            self.dbuf.at[j],
            self.rbuf.at[self.own],
            self.send.at[j],
            self.recv.at[self.own],
            self.place.id(x=j // NYH, yh=lax.rem(j, NYH), c=self.place.l, yl=self.place.c),
        )

    def pair(self, j):
        self.pairing(j).start()

    def pass_on(self, j):
        self.pairing(j).wait_recv()
        total = self.part[self.place.c, j].astype(F32) + self.dbuf[j].astype(F32)
        self.dbuf[j] = total.astype(BF16)
        pl.when(self.away(j))(self.copy(j).start)

        @pl.when(jnp.logical_not(self.away(j)))
        def _():
            self.rbuf[self.own] = self.dbuf[self.own]

    def finish(self):
        total = None
        for j in arrivals(self.place):
            slot = self.rbuf.at[j]
            arrive = sent(slot, slot, self.send.at[0], self.recv.at[j], self.place.partner())
            pl.when(self.away(j))(arrive.wait_recv)
            term = self.rbuf[j].astype(F32)
            total = term if total is None else total + term
        return total

    def end(self):
        for j in range(NB):
            self.pairing(j).wait_send()
            pl.when(self.away(j))(self.copy(j).wait_send)


PARTS = 8


def part_of(width, q):
    tiles = width // 16
    starts = [16 * (tiles * p // PARTS) for p in range(PARTS)] + [width]
    return pl.ds(starts[q], starts[q + 1] - starts[q])


LOOK = 3
LAG = 2


def sum_along_z(place, partial, pbuf, chain, sems, on_part):
    sides = (1, -1)

    def rows(q):
        return part_of(pbuf.shape[2], q)

    def hops(side, q):
        long = (q < PARTS // 2) == (side == 0)
        return 4 if long else 3

    def link(side, k, q, src):
        return sent(
            src,
            chain.at[side, k - 1, :, rows(q), :],
            sems.at[0, side, k - 1, q],
            sems.at[1, side, k - 1, q],
            place.id(z=place.along(sides[side])),
        )

    partial(place.along(4))
    for q in range(PARTS):
        for side in range(2):
            if hops(side, q) == 4:
                link(side, 4, q, pbuf.at[place.along(4), :, rows(q), :]).start()
    for k in (3, 2, 1):
        for side in range(2):
            partial(place.along(k * sides[side]))
            if k == 3:
                j = place.along(k * sides[side])
                for q in range(PARTS):
                    if hops(side, q) == 3:
                        link(side, 3, q, pbuf.at[j, :, rows(q), :]).start()
        for q in range(PARTS):
            for side in range(2):
                j = place.along(k * sides[side])
                if hops(side, q) == 3 and k == 3:
                    continue
                slot = chain.at[side, k, :, rows(q), :]
                link(side, k + 1, q, slot).wait_recv()
                chain[side, k, :, rows(q), :] = (
                    chain[side, k, :, rows(q), :].astype(F32) + pbuf[j, :, rows(q), :].astype(F32)
                ).astype(BF16)
                link(side, k, q, slot).start()
    partial(place.z)
    for q in range(PARTS):
        for side in range(2):
            slot = chain.at[side, 0, :, rows(q), :]
            link(side, 1, q, slot).wait_recv()
        on_part(q, rows(q))
    for q in range(PARTS):
        for side in range(2):
            for k in range(1, hops(side, q) + 1):
                link(side, k, q, chain.at[side, k - 1, :, rows(q), :]).wait_send()


class Ring:
    def __init__(self, place, blocks, sems):
        self.place, self.blocks, self.sems = place, blocks, sems
        self.all = [(q, side) for q in range(PARTS) for side in range(2)]

    def link(self, side, k, q, owner):
        rows = self.blocks.at[owner, part_of(self.blocks.shape[1], q), :]
        step = (1, -1)[side]
        return sent(
            rows,
            rows,
            self.sems.at[0, side, k - 1, q],
            self.sems.at[1, side, k - 1, q],
            self.place.id(z=self.place.along(step)),
        )

    def used(self, side, k, q):
        return k < 4 or (q < PARTS // 2) == (side == 0)

    def start(self, q):
        for side in range(2):
            self.link(side, 1, q, self.place.z).start()

    def run(self, on_arrival):
        on_arrival(self.place.z)
        for k in (1, 2, 3, 4):
            for q, side in self.all:
                if self.used(side, k, q):
                    owner = self.place.along((-k, k)[side])
                    self.link(side, k, q, owner).wait_recv()
                    if k < 4 and self.used(side, k + 1, q):
                        self.link(side, k + 1, q, owner).start()
            on_arrival(self.place.along(-k))
            if k < 4:
                on_arrival(self.place.along(k))

    def end(self):
        for k in (1, 2, 3, 4):
            for q, side in self.all:
                if self.used(side, k, q):
                    self.link(side, k, q, self.place.along((1 - k, k - 1)[side])).wait_send()


def along_order():
    return (4, 3, 5, 2, 6, 1, 7)


def lhs_t(a, b):
    return lax.dot_general(a, b, (((0,), (0,)), ((), ())), preferred_element_type=F32)


def rhs_t(a, b):
    return lax.dot_general(a, b, (((1,), (1,)), ((), ())), preferred_element_type=F32)


def layer_kernel(
    modality, tokens, again, fgain, wq_in, wkv_in, wo_in, wg_in, wu_in, wd_in,
    out,
    xa, gother, fother, gcol, wq, wkv, wo, wg, wu, wd,
    turned, qsend, kvsend, qrecv, kvrecv, ssa, ssar, kvown, kvall, scores, ctxs,
    parta, dbufa, rbufa, resid, src,
    xg, pbuf, chain, ssp, ssr, acts, part, dbuf, rbuf,
    lsem, wsem, ga_sem, q_sem, kv_sem, sa_sem, kz_sem, ky_sem, kr_sem, kd_sem, cx_sem, ra_sem,
    g_sem, c_sem, s_sem, a_sem, r_sem,
):
    place = Place()
    own = place.l
    oth = 1 - place.l
    loads = [
        pltpu.make_async_copy(a, b.at[0], lsem.at[k])
        for k, (a, b) in enumerate(
            ((wq_in, wq), (wkv_in, wkv), (wo_in, wo), (wg_in, wg), (wu_in, wu), (wd_in, wd))
        )
    ]
    for load in loads:
        load.start()
    xd, hd = place.keyval_to()
    xs, hs = place.keyval_from()
    uh, ul = place.up_y()
    dh, dl = place.down_y()
    above = place.id(yh=uh, yl=ul)
    below = place.id(yh=dh, yl=dl)
    twin = place.id(yl=1 - place.l)
    greet(
        place,
        [place.partner(), above, below] + [place.id(z=place.along(k)) for k in range(1, NZ)],
    )

    exchange = []
    for k, (a, b) in enumerate(
        [(again, gother), (wq_in, wq.at[1]), (wkv_in, wkv.at[1]), (wo_in, wo.at[1])]
        + [(w.at[t], v.at[1, t]) for w, v in ((wg_in, wg), (wu_in, wu), (wd_in, wd)) for t in range(2)]
        + [(fgain, fother)]
    ):
        exchange.append(sent(a, b, wsem.at[0, k], wsem.at[1, k], twin))

    rows_in = RowGather(place, tokens, xa, ga_sem)
    for e in exchange[:3] + exchange[10:]:
        e.start()
    rows_in.start()

    def tower_of(j):
        return modality[MODAL_BLOCK * (2 * j + place.l)]

    exchange[0].wait_recv()
    exchange[10].wait_recv()
    for t in range(2):
        for which, pair in enumerate(((again, gother), (fgain, fother))):
            for piece, g in enumerate(pair):
                row = jnp.broadcast_to(g[t : t + 1, :], (MODAL_BLOCK, g.shape[1]))
                gcol[which, piece, t] = jnp.transpose(row)
    for load in loads[:2]:
        load.wait()
    coming = arrivals(place)
    for e in exchange[1:3]:
        e.wait_recv()
    for j in coming[:LOOK]:
        rows_in.forward(j)

    def q_copy(j):
        return sent(
            qsend.at[j], qrecv.at[place.z], q_sem.at[0, j], q_sem.at[1, place.z], place.id(z=j)
        )

    def kv_copy(j):
        return sent(
            kvsend.at[j], kvrecv.at[place.z], kv_sem.at[0, j], kv_sem.at[1, place.z],
            place.id(x=xd, yh=hd, z=j),
        )

    def ssa_copy(j):
        return sent(
            ssa.at[j], ssar.at[place.z], sa_sem.at[0, j], sa_sem.at[1, place.z], place.id(z=j)
        )

    def stays(j):
        return jnp.logical_and(j == place.z, place.moved == 0)

    def send_block(j):
        pl.when(jnp.logical_not(stays(j)))(lambda: kv_copy(j).start())

        @pl.when(stays(j))
        def _():
            kvrecv[place.z] = kvsend[place.z]

        @pl.when(j != place.z)
        def _():
            q_copy(j).start()
            ssa_copy(j).start()

    def squares_of(x0, x1):
        row = jnp.sum(x0 * x0, axis=0, keepdims=True) + jnp.sum(x1 * x1, axis=0, keepdims=True)
        return jnp.broadcast_to(row, (8, MODAL_BLOCK))

    for e in exchange[3:6]:
        e.start()
    for n, j in enumerate(coming):
        if n + LOOK < NB:
            rows_in.forward(coming[n + LOOK])
        rows_in.ready(j)
        tower = tower_of(j)
        x0 = xa[own, j].astype(F32)
        x1 = xa[oth, j].astype(F32)
        ssa[j] = squares_of(x0, x1)
        n0 = (x0 * gcol[0, 0, tower]).astype(BF16)
        n1 = (x1 * gcol[0, 1, tower]).astype(BF16)
        qsend[j] = (lhs_t(wq[0, tower], n0) + lhs_t(wq[1, tower], n1)).astype(BF16)
        kvsend[j] = (
            jnp.dot(wkv[0, tower], n0, preferred_element_type=F32)
            + jnp.dot(wkv[1, tower], n1, preferred_element_type=F32)
        ).astype(BF16)
        send_block(j)

    def turn(side, piece):
        for t in range(2):
            turned[side, piece, t] = jnp.transpose(
                (wg, wu)[side][piece, t].astype(F32)
            ).astype(BF16)

    for side in range(2):
        loads[3 + side].wait()
        turn(side, 0)
    squares = ssa[place.z]
    for k in range(1, NZ):
        slot = ssar.at[place.along(-k)]
        sent(slot, slot, sa_sem.at[0, k], sa_sem.at[1, place.along(-k)], twin).wait_recv()
        squares = squares + ssar[place.along(-k)]
    scale = lax.rsqrt(squares[:1] / D + EPSILON)
    for k in range(NZ):
        slot = kvrecv.at[place.along(-k)]
        wait = sent(slot, slot, kv_sem.at[0, k], kv_sem.at[1, place.along(-k)], twin).wait_recv
        if k:
            wait()
        else:
            pl.when(place.moved != 0)(wait)
    kvown[...] = (jnp.sum(kvrecv[...].astype(F32), axis=0) * scale).astype(BF16)

    kvall[place.h, place.l, place.c, place.z] = kvown[...]

    def kz_copy(k):
        return sent(
            kvown, kvall.at[place.h, place.l, place.c, place.z],
            kz_sem.at[0, k], kz_sem.at[1, k], place.id(z=place.along(k)),
        )

    def ky_copy(side, k, ref):
        return sent(ref, ref, ky_sem.at[0, side, k], ky_sem.at[1, side, k], (above, below)[side])

    def kr_copy(k, ref):
        return sent(ref, ref, kr_sem.at[0, k], kr_sem.at[1, k], (above, below)[k % 2])

    def kd_copy(n, ref):
        return sent(ref, ref, kd_sem.at[0, n], kd_sem.at[1, n], place.partner())

    for k in along_order():
        kz_copy(k).start()
    sources = ((place.h, place.l), (dh, dl), (uh, ul), (1 - place.h, place.l))
    near = (0, 1, 7, 2, 6, 3, 5, 4)

    def piece(n, k):
        h, l = sources[n]
        return kvall.at[h, l, place.c, place.along(-k)]

    for k in near:
        if k:
            sent(piece(0, k), piece(0, k), kz_sem.at[0, k], kz_sem.at[1, k], twin).wait_recv()
        for side in range(2):
            ky_copy(side, k, piece(0, k)).start()
    kd_copy(0, kvall.at[place.h, place.l, place.c]).start()
    qt = qsend[place.z].astype(F32)
    for k in range(1, NZ):
        slot = qrecv.at[place.along(-k)]
        sent(slot, slot, q_sem.at[0, k], q_sem.at[1, place.along(-k)], twin).wait_recv()
        qt = qt + qrecv[place.along(-k)].astype(F32)
    qt = qt * scale
    qt = qt.astype(BF16).astype(F32)
    for k in near:
        ky_copy(0, k, piece(1, k)).wait_recv()
        if k % 2 == 0:
            kr_copy(k, piece(1, k)).start()
        ky_copy(1, k, piece(2, k)).wait_recv()
        if k % 2 == 1:
            kr_copy(k, piece(2, k)).start()
    for n in (1, 2):
        kd_copy(n, kvall.at[sources[n][0], sources[n][1], place.c]).start()
    for k in near:
        kr_copy(k, piece(3, k)).wait_recv()
    kd_copy(3, kvall.at[sources[3][0], sources[3][1], place.c]).start()
    for e in exchange[6:8]:
        e.start()
    for n in range(4):
        slot = kvall.at[sources[n][0], sources[n][1], 1 - place.c]
        kd_copy(n, slot).wait_recv()

    qblock = 2 * place.z + place.l

    def keyval(kind, l, z):
        return jnp.concatenate((kvall[kind, l, 0, z], kvall[kind, l, 1, z]), axis=0)

    shape = (MODAL_BLOCK, MODAL_BLOCK)
    query = jnp.transpose(qt).astype(BF16)
    ahead = lax.broadcasted_iota(jnp.int32, shape, 1) - lax.broadcasted_iota(jnp.int32, shape, 0)
    largest = jnp.full(shape, -1e30, F32)
    for z in range(NZ):
        for l in range(2):
            b = 2 * z + l
            s = jnp.dot(query, keyval(0, l, z), preferred_element_type=F32) * HD ** (-0.5)
            s = jnp.where(ahead <= (qblock - b) * MODAL_BLOCK, s, -1e30)
            scores[b] = s
            largest = jnp.maximum(largest, s)
    largest = jnp.max(largest, axis=1, keepdims=True)
    norm = jnp.zeros(shape, F32)
    for b in range(2 * NZ):
        p = jnp.exp(scores[b] - largest)
        scores[b] = p
        norm = norm + p
    inverse = 1.0 / jnp.sum(norm, axis=1, keepdims=True)
    ctx = jnp.zeros((MODAL_BLOCK, HD), F32)
    for z in range(NZ):
        for l in range(2):
            p = (scores[2 * z + l] * inverse).astype(BF16)
            ctx = ctx + rhs_t(p, keyval(1, l, z))
    ctxs[place.z] = jnp.transpose(ctx).astype(BF16)

    def cx(k, owner):
        first = 64 if k == -4 else 0
        ref = ctxs.at[owner, pl.ds(first, HD // 2 if abs(k) == 4 else HD), :]
        n = 0 if k == -4 else k % NZ
        step = {3: 1, -3: -1, 4: 2, -4: -2}.get(k, k)
        return sent(ref, ref, cx_sem.at[0, n], cx_sem.at[1, n], place.id(z=place.along(step)))

    for k in (2, -2, 1, -1):
        cx(k, place.z).start()
    for e in exchange[4:6]:
        e.wait_recv()
    turn(0, 1)
    loads[2].wait()
    exchange[3].wait_recv()
    rows_out = RowSum(place, parta, dbufa, rbufa, ra_sem)

    def outward(j):
        tower = tower_of(j)
        parta[own, j] = jnp.dot(wo[0, tower], ctxs[j], preferred_element_type=F32).astype(BF16)
        parta[oth, j] = jnp.dot(wo[1, tower], ctxs[j], preferred_element_type=F32).astype(BF16)
        rows_out.pair(j)

    outward(place.z)
    for side in (1, -1):
        owner = place.along(-2 * side)
        cx(2 * side, owner).wait_recv()
        cx(3 * side, owner).start()
        cx(4 * side, owner).start()
    sums = [place.z]
    for k in (1, -1, 2, -2, 3, -3, 4):
        j = place.along(-k)
        if abs(k) != 2:
            cx(k, j).wait_recv()
        if k == 4:
            cx(-4, j).wait_recv()
        outward(j)
        if len(sums) >= LAG:
            rows_out.pass_on(sums[-LAG])
        sums.append(j)
    for j in sums[-LAG:]:
        rows_out.pass_on(j)
    resid[...] = tokens[...].astype(F32) + rows_out.finish()

    src[...] = resid[...].astype(BF16)
    rows_mid = RowGather(place, src, xg, g_sem)
    rows_mid.start()
    for e in exchange[6:8]:
        e.wait_recv()
    turn(1, 1)
    needed = [place.along(k) for k in (4, 3, -3, 2, -2, 1, -1, 0)]
    for j in needed[:LOOK]:
        rows_mid.forward(j)
    for e in exchange[8:10]:
        e.start()

    def squares_to(k):
        j = place.along(k)
        return sent(ssp.at[j], ssr.at[place.z], s_sem.at[0, k], s_sem.at[1, k], place.id(z=j))

    called = []

    def partial(j):
        n = len(called)
        called.append(j)
        if n + LOOK < NB:
            rows_mid.forward(needed[n + LOOK])
        rows_mid.ready(needed[n])
        tower = tower_of(j)
        x0 = xg[own, j].astype(F32)
        x1 = xg[oth, j].astype(F32)
        ssp[j] = squares_of(x0, x1)
        n0 = (x0 * gcol[1, 0, tower]).astype(BF16)
        n1 = (x1 * gcol[1, 1, tower]).astype(BF16)
        for side in range(2):
            pbuf[j, side] = (
                jnp.dot(turned[side, 0, tower], n0, preferred_element_type=F32)
                + jnp.dot(turned[side, 1, tower], n1, preferred_element_type=F32)
            ).astype(BF16)
        if n + 1 < NB:
            squares_to((4, 3, -3, 2, -2, 1, -1)[n] % NZ).start()

    ring = Ring(place, acts, a_sem)
    scales = []

    def activate(q, rows):
        if not scales:
            squares = ssp[place.z]
            for k in range(1, NZ):
                slot = ssr.at[place.along(-k)]
                sent(slot, slot, s_sem.at[0, k], s_sem.at[1, k], twin).wait_recv()
                squares = squares + ssr[place.along(-k)]
            scales.append(lax.rsqrt(squares[:1] / D + EPSILON))
        gate, up = (
            (
                pbuf[place.z, side, rows, :].astype(F32)
                + chain[0, 0, side, rows, :].astype(F32)
                + chain[1, 0, side, rows, :].astype(F32)
            )
            * scales[0]
            for side in range(2)
        )
        acts[place.z, rows, :] = (gate / (1.0 + jnp.exp(-gate)) * up).astype(BF16)
        ring.start(q)

    sum_along_z(place, partial, pbuf, chain, c_sem, activate)
    loads[5].wait()
    for e in exchange[8:10]:
        e.wait_recv()
    rows_end = RowSum(place, part, dbuf, rbuf, r_sem)
    done = []

    def downward(j):
        tower = tower_of(j)
        act = acts[j]
        part[own, j] = jnp.dot(wd[0, tower], act, preferred_element_type=F32).astype(BF16)
        part[oth, j] = jnp.dot(wd[1, tower], act, preferred_element_type=F32).astype(BF16)
        rows_end.pair(j)
        if len(done) >= LAG:
            rows_end.pass_on(done[-LAG])
        done.append(j)

    ring.run(downward)
    for j in done[-LAG:]:
        rows_end.pass_on(j)
    total = rows_end.finish()
    out[...] = (resid[...] + total).astype(BF16)

    ring.end()
    rows_in.end()
    rows_mid.end()
    rows_out.end()
    rows_end.end()
    for e in exchange:
        e.wait_send()
    for k in range(1, NZ):
        j = place.along(k)
        squares_to(k).wait_send()
        q_copy(j).wait_send()
        kv_copy(j).wait_send()
        ssa_copy(j).wait_send()
        kz_copy(k).wait_send()
    for side in (1, -1):
        for k in (1, 2):
            cx(k * side, place.z).wait_send()
        for k in (3, 4):
            cx(k * side, place.along(-2 * side)).wait_send()
    pl.when(place.moved != 0)(kv_copy(place.z).wait_send)
    for k in range(NZ):
        for side in range(2):
            ky_copy(side, k, piece(0, k)).wait_send()
        kr_copy(k, piece(1 + k % 2, k)).wait_send()
    for n in range(4):
        kd_copy(n, kvall.at[sources[n][0], sources[n][1], place.c]).wait_send()


def local(tokens, modality, attn_gain, ffn_gain, w_query, w_keyval, w_out, w_gate, w_up, w_down):
    feats = tokens.shape[1]
    width = w_gate.shape[2]
    kvw = w_keyval.shape[2]
    vmem = pl.BlockSpec(memory_space=pltpu.VMEM)
    hbm = pl.BlockSpec(memory_space=pltpu.HBM)
    smem = pl.BlockSpec(memory_space=pltpu.SMEM)
    dma = pltpu.SemaphoreType.DMA
    rows = (feats, MODAL_BLOCK)
    result = pl.pallas_call(
        layer_kernel,
        out_shape=jax.ShapeDtypeStruct(rows, BF16),
        in_specs=[smem, vmem, vmem, vmem] + [hbm] * 6,
        out_specs=vmem,
        scratch_shapes=[
            pltpu.VMEM((2, NB, *rows), BF16),
            pltpu.VMEM((2, feats), F32),
            pltpu.VMEM((2, feats), F32),
            pltpu.VMEM((2, 2, 2, *rows), F32),
            pltpu.VMEM((2, 2, feats, HD), BF16),
            pltpu.VMEM((2, 2, kvw, feats), BF16),
            pltpu.VMEM((2, 2, feats, HD), BF16),
            pltpu.VMEM((2, 2, feats, width), BF16),
            pltpu.VMEM((2, 2, feats, width), BF16),
            pltpu.VMEM((2, 2, feats, width), BF16),
            pltpu.VMEM((2, 2, 2, width, feats), BF16),
            pltpu.VMEM((NZ, HD, MODAL_BLOCK), BF16),
            pltpu.VMEM((NZ, kvw, MODAL_BLOCK), BF16),
            pltpu.VMEM((NZ, HD, MODAL_BLOCK), BF16),
            pltpu.VMEM((NZ, kvw, MODAL_BLOCK), BF16),
            pltpu.VMEM((NZ, 8, MODAL_BLOCK), F32),
            pltpu.VMEM((NZ, 8, MODAL_BLOCK), F32),
            pltpu.VMEM((kvw, MODAL_BLOCK), BF16),
            pltpu.VMEM((2, 2, 2, NZ, kvw, MODAL_BLOCK), BF16),
            pltpu.VMEM((2 * NZ, MODAL_BLOCK, MODAL_BLOCK), F32),
            pltpu.VMEM((NZ, HD, MODAL_BLOCK), BF16),
            pltpu.VMEM((2, NB, *rows), BF16),
            pltpu.VMEM((NB, *rows), BF16),
            pltpu.VMEM((NB, *rows), BF16),
            pltpu.VMEM(rows, F32),
            pltpu.VMEM(rows, BF16),
            pltpu.VMEM((2, NB, *rows), BF16),
            pltpu.VMEM((NZ, 2, width, MODAL_BLOCK), BF16),
            pltpu.VMEM((2, 4, 2, width, MODAL_BLOCK), BF16),
            pltpu.VMEM((NZ, 8, MODAL_BLOCK), F32),
            pltpu.VMEM((NZ, 8, MODAL_BLOCK), F32),
            pltpu.VMEM((NZ, width, MODAL_BLOCK), BF16),
            pltpu.VMEM((2, NB, *rows), BF16),
            pltpu.VMEM((NB, *rows), BF16),
            pltpu.VMEM((NB, *rows), BF16),
            dma((6,)),
            dma((2, 11)),
            dma((4, NB)),
            dma((2, NZ)),
            dma((2, NZ)),
            dma((2, NZ)),
            dma((2, NZ)),
            dma((2, 2, NZ)),
            dma((2, NZ)),
            dma((2, 4)),
            dma((2, NZ)),
            dma((4, NB)),
            dma((4, NB)),
            dma((2, 2, 4, PARTS)),
            dma((2, NZ)),
            dma((2, 2, 4, PARTS)),
            dma((4, NB)),
        ],
        compiler_params=pltpu.CompilerParams(collective_id=0, has_side_effects=True),
        name="layer",
    )(
        modality,
        tokens.T,
        attn_gain,
        ffn_gain,
        w_query,
        jnp.swapaxes(w_keyval, 1, 2),
        jnp.swapaxes(w_out, 1, 2),
        w_gate,
        w_up,
        jnp.swapaxes(w_down, 1, 2),
    )
    return result.T


def solution(mesh):
    torus = Mesh(mesh.devices.reshape(NX, NYH, 2, 2, NZ), AXES)
    in_specs = (
        P(ROWS, MP),
        P(),
        P(None, MP),
        P(None, MP),
        P(None, MP, ROWS),
        P(None, MP, ROWS),
        P(None, ROWS, MP),
        P(None, MP, ROWS),
        P(None, MP, ROWS),
        P(None, ROWS, MP),
    )
    out_specs = P(ROWS, MP)
    return jax.shard_map(local, mesh=torus, in_specs=in_specs, out_specs=out_specs, check_vma=False)
```

```python
import jax
import jax.numpy as jnp
from jax import lax
from jax.experimental import pallas as pl
from jax.experimental.pallas import tpu as pltpu
from jax.sharding import Mesh
from jax.sharding import PartitionSpec as P

D = 3584
HD = 128
MODAL_BLOCK = 128
ROWS = ("x", "yh", "c")
MP = ("yl", "z")
AXES = ("x", "yh", "c", "yl", "z")
NX, NYH, NZ = 4, 2, 8
NB = NX * NYH

EPSILON = 1e-06
F32 = jnp.float32
BF16 = jnp.bfloat16


class Place:
    def __init__(self):
        self.at = {a: lax.axis_index(a) for a in AXES}
        self.x, self.h, self.c, self.l, self.z = (self.at[a] for a in AXES)
        self.crossed = (self.c - self.l) * (self.c - self.l)
        xa, xb = self.x // NYH, lax.rem(self.x, NYH)
        self.moved = 1 - (1 - (xa - xb) * (xa - xb)) * (1 - (xb - self.h) * (xb - self.h))

    def id(self, **moved):
        return tuple(moved.get(a, self.at[a]) for a in AXES)

    def cross(self, dx, dh):
        return self.id(
            x=lax.rem(self.x + dx, NX), yh=lax.rem(self.h + dh, NYH), c=self.l, yl=self.c
        )

    def ahead(self, dx, dh):
        return NYH * lax.rem(self.x + dx, NX) + lax.rem(self.h + dh, NYH)

    def behind(self, dx, dh):
        return NYH * lax.rem(self.x - dx + NX, NX) + lax.rem(self.h - dh + NYH, NYH)

    def partner(self):
        return self.id(c=1 - self.c)

    def along(self, k):
        return lax.rem(self.z + k + NZ, NZ)

    def up_y(self):
        return lax.rem(self.h + self.l, NYH), 1 - self.l

    def down_y(self):
        return lax.rem(self.h + 1 - self.l, NYH), 1 - self.l

    def keyval_to(self):
        return NYH * lax.rem(self.x, NYH) + self.h, self.x // NYH

    def keyval_from(self):
        return NYH * self.h + self.x // NYH, lax.rem(self.x, NYH)


OFFSETS = tuple((dx, dh) for dx in (1, 3, 2, 0) for dh in (1, 0))


def sent(src, dst, send, recv, target):
    return pltpu.make_async_remote_copy(
        src_ref=src,
        dst_ref=dst,
        send_sem=send,
        recv_sem=recv,
        device_id=target,
        device_id_type=pl.DeviceIdType.MESH,
    )


def greet(place, peers):
    barrier = pltpu.get_barrier_semaphore()

    def hello(peer):
        pl.semaphore_signal(barrier, 1, device_id=peer, device_id_type=pl.DeviceIdType.MESH)

    count = 0
    for peer in peers + [place.cross(*o) for o in OFFSETS if o != (0, 0)]:
        hello(peer)
        count += 1
    xs, hs = place.keyval_from()
    for k in range(1, NZ):
        hello(place.id(x=xs, yh=hs, z=place.along(k)))
        count += 1
    pl.when(place.c != place.l)(lambda: hello(place.cross(0, 0)))
    pl.when(place.moved != 0)(lambda: hello(place.id(x=xs, yh=hs)))
    pl.semaphore_wait(barrier, count + place.crossed + place.moved)


def arrivals(place):
    order = sorted(OFFSETS, key=lambda o: (min(o[0], NX - o[0]), o[1]))
    return [place.behind(*o) for o in order]


class RowGather:
    def __init__(self, place, src, xg, sems):
        self.place, self.src, self.xg = place, src, xg
        self.send, self.recv, self.fsend, self.frecv = (sems.at[k] for k in range(4))
        self.own = NYH * place.x + place.h

    def away(self, j):
        return jnp.logical_or(j != self.own, self.place.c != self.place.l)

    def copy(self, i):
        return sent(
            self.src,
            self.xg.at[self.place.l, self.own],
            self.send.at[i],
            self.recv.at[self.own],
            self.place.cross(*OFFSETS[i]),
        )

    def start(self):
        place = self.place
        for i, offset in enumerate(OFFSETS):
            if offset != (0, 0):
                self.copy(i).start()
            else:
                pl.when(place.c != place.l)(self.copy(i).start)

                @pl.when(place.c == place.l)
                def _():
                    self.xg[place.l, self.own] = self.src[...]

    def forwarding(self, j, piece):
        slot = self.xg.at[piece, j]
        return sent(slot, slot, self.fsend.at[j], self.frecv.at[j], self.place.partner())

    def forward(self, j):
        slot = self.xg.at[self.place.c, j]
        arrive = sent(slot, slot, self.send.at[0], self.recv.at[j], self.place.partner())
        pl.when(self.away(j))(arrive.wait_recv)
        self.forwarding(j, self.place.c).start()

    def ready(self, j):
        self.forwarding(j, 1 - self.place.c).wait_recv()

    def end(self):
        for i, offset in enumerate(OFFSETS):
            if offset != (0, 0):
                self.copy(i).wait_send()
            else:
                pl.when(self.place.c != self.place.l)(self.copy(i).wait_send)
        for j in range(NB):
            self.forwarding(j, self.place.c).wait_send()


class RowSum:
    def __init__(self, place, part, dbuf, rbuf, sems):
        self.place, self.part, self.dbuf, self.rbuf = place, part, dbuf, rbuf
        self.send, self.recv, self.fsend, self.frecv = (sems.at[k] for k in range(4))
        self.own = NYH * place.x + place.h

    def away(self, j):
        return jnp.logical_or(j != self.own, self.place.c != self.place.l)

    def pairing(self, j):
        return sent(
            self.part.at[1 - self.place.c, j],
            self.dbuf.at[j],
            self.fsend.at[j],
            self.frecv.at[j],
            self.place.partner(),
        )

    def copy(self, j):
        return sent(
            self.dbuf.at[j],
            self.rbuf.at[self.own],
            self.send.at[j],
            self.recv.at[self.own],
            self.place.id(x=j // NYH, yh=lax.rem(j, NYH), c=self.place.l, yl=self.place.c),
        )

    def pair(self, j):
        self.pairing(j).start()

    def pass_on(self, j):
        self.pairing(j).wait_recv()
        total = self.part[self.place.c, j].astype(F32) + self.dbuf[j].astype(F32)
        self.dbuf[j] = total.astype(BF16)
        pl.when(self.away(j))(self.copy(j).start)

        @pl.when(jnp.logical_not(self.away(j)))
        def _():
            self.rbuf[self.own] = self.dbuf[self.own]

    def finish(self):
        total = None
        for j in arrivals(self.place):
            slot = self.rbuf.at[j]
            arrive = sent(slot, slot, self.send.at[0], self.recv.at[j], self.place.partner())
            pl.when(self.away(j))(arrive.wait_recv)
            term = self.rbuf[j].astype(F32)
            total = term if total is None else total + term
        return total

    def end(self):
        for j in range(NB):
            self.pairing(j).wait_send()
            pl.when(self.away(j))(self.copy(j).wait_send)


PARTS = 8


def part_of(width, q):
    tiles = width // 16
    starts = [16 * (tiles * p // PARTS) for p in range(PARTS)] + [width]
    return pl.ds(starts[q], starts[q + 1] - starts[q])


LOOK = 3
LAG = 3


def sum_along_z(place, partial, pbuf, chain, sems, on_part):
    sides = (1, -1)

    def rows(q):
        return part_of(pbuf.shape[2], q)

    def hops(side, q):
        long = (q < PARTS // 2) == (side == 0)
        return 4 if long else 3

    def link(side, k, q, src):
        return sent(
            src,
            chain.at[side, k - 1, :, rows(q), :],
            sems.at[0, side, k - 1, q],
            sems.at[1, side, k - 1, q],
            place.id(z=place.along(sides[side])),
        )

    partial(place.along(4))
    for q in range(PARTS):
        for side in range(2):
            if hops(side, q) == 4:
                link(side, 4, q, pbuf.at[place.along(4), :, rows(q), :]).start()
    for k in (3, 2, 1):
        for side in range(2):
            partial(place.along(k * sides[side]))
            if k == 3:
                j = place.along(k * sides[side])
                for q in range(PARTS):
                    if hops(side, q) == 3:
                        link(side, 3, q, pbuf.at[j, :, rows(q), :]).start()
        for q in range(PARTS):
            for side in range(2):
                j = place.along(k * sides[side])
                if hops(side, q) == 3 and k == 3:
                    continue
                slot = chain.at[side, k, :, rows(q), :]
                link(side, k + 1, q, slot).wait_recv()
                chain[side, k, :, rows(q), :] = (
                    chain[side, k, :, rows(q), :].astype(F32) + pbuf[j, :, rows(q), :].astype(F32)
                ).astype(BF16)
                link(side, k, q, slot).start()
    partial(place.z)
    for q in range(PARTS):
        for side in range(2):
            slot = chain.at[side, 0, :, rows(q), :]
            link(side, 1, q, slot).wait_recv()
        on_part(q, rows(q))
    for q in range(PARTS):
        for side in range(2):
            for k in range(1, hops(side, q) + 1):
                link(side, k, q, chain.at[side, k - 1, :, rows(q), :]).wait_send()


class Ring:
    def __init__(self, place, blocks, sems):
        self.place, self.blocks, self.sems = place, blocks, sems
        self.all = [(q, side) for q in range(PARTS) for side in range(2)]

    def link(self, side, k, q, owner):
        rows = self.blocks.at[owner, part_of(self.blocks.shape[1], q), :]
        step = (1, -1)[side]
        return sent(
            rows,
            rows,
            self.sems.at[0, side, k - 1, q],
            self.sems.at[1, side, k - 1, q],
            self.place.id(z=self.place.along(step)),
        )

    def used(self, side, k, q):
        return k < 4 or (q < PARTS // 2) == (side == 0)

    def start(self, q):
        for side in range(2):
            self.link(side, 1, q, self.place.z).start()

    def run(self, on_arrival):
        on_arrival(self.place.z)
        for k in (1, 2, 3, 4):
            for q, side in self.all:
                if self.used(side, k, q):
                    owner = self.place.along((-k, k)[side])
                    self.link(side, k, q, owner).wait_recv()
                    if k < 4 and self.used(side, k + 1, q):
                        self.link(side, k + 1, q, owner).start()
            on_arrival(self.place.along(-k))
            if k < 4:
                on_arrival(self.place.along(k))

    def end(self):
        for k in (1, 2, 3, 4):
            for q, side in self.all:
                if self.used(side, k, q):
                    self.link(side, k, q, self.place.along((1 - k, k - 1)[side])).wait_send()


def along_order():
    return (4, 3, 5, 2, 6, 1, 7)


def lhs_t(a, b):
    return lax.dot_general(a, b, (((0,), (0,)), ((), ())), preferred_element_type=F32)


def rhs_t(a, b):
    return lax.dot_general(a, b, (((1,), (1,)), ((), ())), preferred_element_type=F32)


def layer_kernel(
    modality, tokens, again, fgain, wq_in, wkv_in, wo_in, wg_in, wu_in, wd_in,
    out,
    xa, gother, fother, gcol, wq, wkv, wo, wg, wu, wd,
    turned, qsend, kvsend, qrecv, kvrecv, ssa, ssar, kvown, kvall, scores, ctxs,
    parta, dbufa, rbufa, resid, src,
    xg, pbuf, chain, ssp, ssr, acts, part, dbuf, rbuf,
    lsem, wsem, ga_sem, q_sem, kv_sem, sa_sem, kz_sem, ky_sem, kr_sem, kd_sem, cx_sem, ra_sem,
    g_sem, c_sem, s_sem, a_sem, r_sem,
):
    place = Place()
    own = place.l
    oth = 1 - place.l
    loads = [
        pltpu.make_async_copy(a, b.at[0], lsem.at[k])
        for k, (a, b) in enumerate(
            ((wq_in, wq), (wkv_in, wkv), (wo_in, wo), (wg_in, wg), (wu_in, wu), (wd_in, wd))
        )
    ]
    for load in loads:
        load.start()
    xd, hd = place.keyval_to()
    xs, hs = place.keyval_from()
    uh, ul = place.up_y()
    dh, dl = place.down_y()
    above = place.id(yh=uh, yl=ul)
    below = place.id(yh=dh, yl=dl)
    twin = place.id(yl=1 - place.l)
    greet(
        place,
        [place.partner(), above, below] + [place.id(z=place.along(k)) for k in range(1, NZ)],
    )

    exchange = []
    for k, (a, b) in enumerate(
        [(again, gother), (wq_in, wq.at[1]), (wkv_in, wkv.at[1]), (wo_in, wo.at[1])]
        + [(w.at[t], v.at[1, t]) for w, v in ((wg_in, wg), (wu_in, wu), (wd_in, wd)) for t in range(2)]
        + [(fgain, fother)]
    ):
        exchange.append(sent(a, b, wsem.at[0, k], wsem.at[1, k], twin))

    rows_in = RowGather(place, tokens, xa, ga_sem)
    for e in exchange[:3] + exchange[10:]:
        e.start()
    rows_in.start()

    def tower_of(j):
        return modality[MODAL_BLOCK * (2 * j + place.l)]

    exchange[0].wait_recv()
    exchange[10].wait_recv()
    for t in range(2):
        for which, pair in enumerate(((again, gother), (fgain, fother))):
            for piece, g in enumerate(pair):
                row = jnp.broadcast_to(g[t : t + 1, :], (MODAL_BLOCK, g.shape[1]))
                gcol[which, piece, t] = jnp.transpose(row)
    for load in loads[:2]:
        load.wait()
    coming = arrivals(place)
    for e in exchange[1:3]:
        e.wait_recv()
    for j in coming[:LOOK]:
        rows_in.forward(j)

    def q_copy(j):
        return sent(
            qsend.at[j], qrecv.at[place.z], q_sem.at[0, j], q_sem.at[1, place.z], place.id(z=j)
        )

    def kv_copy(j):
        return sent(
            kvsend.at[j], kvrecv.at[place.z], kv_sem.at[0, j], kv_sem.at[1, place.z],
            place.id(x=xd, yh=hd, z=j),
        )

    def ssa_copy(j):
        return sent(
            ssa.at[j], ssar.at[place.z], sa_sem.at[0, j], sa_sem.at[1, place.z], place.id(z=j)
        )

    def stays(j):
        return jnp.logical_and(j == place.z, place.moved == 0)

    def send_block(j):
        pl.when(jnp.logical_not(stays(j)))(lambda: kv_copy(j).start())

        @pl.when(stays(j))
        def _():
            kvrecv[place.z] = kvsend[place.z]

        @pl.when(j != place.z)
        def _():
            q_copy(j).start()
            ssa_copy(j).start()

    def squares_of(x0, x1):
        row = jnp.sum(x0 * x0, axis=0, keepdims=True) + jnp.sum(x1 * x1, axis=0, keepdims=True)
        return jnp.broadcast_to(row, (8, MODAL_BLOCK))

    for e in exchange[3:6]:
        e.start()
    for n, j in enumerate(coming):
        if n + LOOK < NB:
            rows_in.forward(coming[n + LOOK])
        rows_in.ready(j)
        tower = tower_of(j)
        x0 = xa[own, j].astype(F32)
        x1 = xa[oth, j].astype(F32)
        ssa[j] = squares_of(x0, x1)
        n0 = (x0 * gcol[0, 0, tower]).astype(BF16)
        n1 = (x1 * gcol[0, 1, tower]).astype(BF16)
        qsend[j] = (lhs_t(wq[0, tower], n0) + lhs_t(wq[1, tower], n1)).astype(BF16)
        kvsend[j] = (
            jnp.dot(wkv[0, tower], n0, preferred_element_type=F32)
            + jnp.dot(wkv[1, tower], n1, preferred_element_type=F32)
        ).astype(BF16)
        send_block(j)

    def turn(side, piece):
        for t in range(2):
            turned[side, piece, t] = jnp.transpose(
                (wg, wu)[side][piece, t].astype(F32)
            ).astype(BF16)

    for side in range(2):
        loads[3 + side].wait()
        turn(side, 0)
    squares = ssa[place.z]
    for k in range(1, NZ):
        slot = ssar.at[place.along(-k)]
        sent(slot, slot, sa_sem.at[0, k], sa_sem.at[1, place.along(-k)], twin).wait_recv()
        squares = squares + ssar[place.along(-k)]
    scale = lax.rsqrt(squares[:1] / D + EPSILON)
    for k in range(NZ):
        slot = kvrecv.at[place.along(-k)]
        wait = sent(slot, slot, kv_sem.at[0, k], kv_sem.at[1, place.along(-k)], twin).wait_recv
        if k:
            wait()
        else:
            pl.when(place.moved != 0)(wait)
    kvown[...] = (jnp.sum(kvrecv[...].astype(F32), axis=0) * scale).astype(BF16)

    kvall[place.h, place.l, place.c, place.z] = kvown[...]

    def kz_copy(k):
        return sent(
            kvown, kvall.at[place.h, place.l, place.c, place.z],
            kz_sem.at[0, k], kz_sem.at[1, k], place.id(z=place.along(k)),
        )

    def ky_copy(side, k, ref):
        return sent(ref, ref, ky_sem.at[0, side, k], ky_sem.at[1, side, k], (above, below)[side])

    def kr_copy(k, ref):
        return sent(ref, ref, kr_sem.at[0, k], kr_sem.at[1, k], (above, below)[k % 2])

    def kd_copy(n, ref):
        return sent(ref, ref, kd_sem.at[0, n], kd_sem.at[1, n], place.partner())

    for k in along_order():
        kz_copy(k).start()
    sources = ((place.h, place.l), (dh, dl), (uh, ul), (1 - place.h, place.l))
    near = (0, 1, 7, 2, 6, 3, 5, 4)

    def piece(n, k):
        h, l = sources[n]
        return kvall.at[h, l, place.c, place.along(-k)]

    for k in near:
        if k:
            sent(piece(0, k), piece(0, k), kz_sem.at[0, k], kz_sem.at[1, k], twin).wait_recv()
        for side in range(2):
            ky_copy(side, k, piece(0, k)).start()
    kd_copy(0, kvall.at[place.h, place.l, place.c]).start()
    qt = qsend[place.z].astype(F32)
    for k in range(1, NZ):
        slot = qrecv.at[place.along(-k)]
        sent(slot, slot, q_sem.at[0, k], q_sem.at[1, place.along(-k)], twin).wait_recv()
        qt = qt + qrecv[place.along(-k)].astype(F32)
    qt = qt * scale
    qt = qt.astype(BF16).astype(F32)
    for k in near:
        ky_copy(0, k, piece(1, k)).wait_recv()
        if k % 2 == 0:
            kr_copy(k, piece(1, k)).start()
        ky_copy(1, k, piece(2, k)).wait_recv()
        if k % 2 == 1:
            kr_copy(k, piece(2, k)).start()
    for n in (1, 2):
        kd_copy(n, kvall.at[sources[n][0], sources[n][1], place.c]).start()
    for k in near:
        kr_copy(k, piece(3, k)).wait_recv()
    kd_copy(3, kvall.at[sources[3][0], sources[3][1], place.c]).start()
    for e in exchange[6:8]:
        e.start()
    for n in range(4):
        slot = kvall.at[sources[n][0], sources[n][1], 1 - place.c]
        kd_copy(n, slot).wait_recv()

    qblock = 2 * place.z + place.l

    def keyval(kind, l, z):
        return jnp.concatenate((kvall[kind, l, 0, z], kvall[kind, l, 1, z]), axis=0)

    shape = (MODAL_BLOCK, MODAL_BLOCK)
    query = jnp.transpose(qt).astype(BF16)
    ahead = lax.broadcasted_iota(jnp.int32, shape, 1) - lax.broadcasted_iota(jnp.int32, shape, 0)
    largest = jnp.full(shape, -1e30, F32)
    for z in range(NZ):
        for l in range(2):
            b = 2 * z + l
            s = jnp.dot(query, keyval(0, l, z), preferred_element_type=F32) * HD ** (-0.5)
            s = jnp.where(ahead <= (qblock - b) * MODAL_BLOCK, s, -1e30)
            scores[b] = s
            largest = jnp.maximum(largest, s)
    largest = jnp.max(largest, axis=1, keepdims=True)
    norm = jnp.zeros(shape, F32)
    for b in range(2 * NZ):
        p = jnp.exp(scores[b] - largest)
        scores[b] = p
        norm = norm + p
    inverse = 1.0 / jnp.sum(norm, axis=1, keepdims=True)
    ctx = jnp.zeros((MODAL_BLOCK, HD), F32)
    for z in range(NZ):
        for l in range(2):
            p = (scores[2 * z + l] * inverse).astype(BF16)
            ctx = ctx + rhs_t(p, keyval(1, l, z))
    ctxs[place.z] = jnp.transpose(ctx).astype(BF16)

    def cx(k, owner):
        first = 64 if k == -4 else 0
        ref = ctxs.at[owner, pl.ds(first, HD // 2 if abs(k) == 4 else HD), :]
        n = 0 if k == -4 else k % NZ
        step = {3: 1, -3: -1, 4: 2, -4: -2}.get(k, k)
        return sent(ref, ref, cx_sem.at[0, n], cx_sem.at[1, n], place.id(z=place.along(step)))

    for k in (2, -2, 1, -1):
        cx(k, place.z).start()
    for e in exchange[4:6]:
        e.wait_recv()
    turn(0, 1)
    loads[2].wait()
    exchange[3].wait_recv()
    rows_out = RowSum(place, parta, dbufa, rbufa, ra_sem)

    def outward(j):
        tower = tower_of(j)
        parta[own, j] = jnp.dot(wo[0, tower], ctxs[j], preferred_element_type=F32).astype(BF16)
        parta[oth, j] = jnp.dot(wo[1, tower], ctxs[j], preferred_element_type=F32).astype(BF16)
        rows_out.pair(j)

    outward(place.z)
    for side in (1, -1):
        owner = place.along(-2 * side)
        cx(2 * side, owner).wait_recv()
        cx(3 * side, owner).start()
        cx(4 * side, owner).start()
    sums = [place.z]
    for k in (1, -1, 2, -2, 3, -3, 4):
        j = place.along(-k)
        if abs(k) != 2:
            cx(k, j).wait_recv()
        if k == 4:
            cx(-4, j).wait_recv()
        outward(j)
        if len(sums) >= LAG:
            rows_out.pass_on(sums[-LAG])
        sums.append(j)
    for j in sums[-LAG:]:
        rows_out.pass_on(j)
    resid[...] = tokens[...].astype(F32) + rows_out.finish()

    src[...] = resid[...].astype(BF16)
    rows_mid = RowGather(place, src, xg, g_sem)
    rows_mid.start()
    for e in exchange[6:8]:
        e.wait_recv()
    turn(1, 1)
    needed = [place.along(k) for k in (4, 3, -3, 2, -2, 1, -1, 0)]
    for j in needed[:LOOK]:
        rows_mid.forward(j)
    for e in exchange[8:10]:
        e.start()

    def squares_to(k):
        j = place.along(k)
        return sent(ssp.at[j], ssr.at[place.z], s_sem.at[0, k], s_sem.at[1, k], place.id(z=j))

    called = []

    def partial(j):
        n = len(called)
        called.append(j)
        if n + LOOK < NB:
            rows_mid.forward(needed[n + LOOK])
        rows_mid.ready(needed[n])
        tower = tower_of(j)
        x0 = xg[own, j].astype(F32)
        x1 = xg[oth, j].astype(F32)
        ssp[j] = squares_of(x0, x1)
        n0 = (x0 * gcol[1, 0, tower]).astype(BF16)
        n1 = (x1 * gcol[1, 1, tower]).astype(BF16)
        for side in range(2):
            pbuf[j, side] = (
                jnp.dot(turned[side, 0, tower], n0, preferred_element_type=F32)
                + jnp.dot(turned[side, 1, tower], n1, preferred_element_type=F32)
            ).astype(BF16)
        if n + 1 < NB:
            squares_to((4, 3, -3, 2, -2, 1, -1)[n] % NZ).start()

    ring = Ring(place, acts, a_sem)
    scales = []

    def activate(q, rows):
        if not scales:
            squares = ssp[place.z]
            for k in range(1, NZ):
                slot = ssr.at[place.along(-k)]
                sent(slot, slot, s_sem.at[0, k], s_sem.at[1, k], twin).wait_recv()
                squares = squares + ssr[place.along(-k)]
            scales.append(lax.rsqrt(squares[:1] / D + EPSILON))
        gate, up = (
            (
                pbuf[place.z, side, rows, :].astype(F32)
                + chain[0, 0, side, rows, :].astype(F32)
                + chain[1, 0, side, rows, :].astype(F32)
            )
            * scales[0]
            for side in range(2)
        )
        acts[place.z, rows, :] = (gate / (1.0 + jnp.exp(-gate)) * up).astype(BF16)
        ring.start(q)

    sum_along_z(place, partial, pbuf, chain, c_sem, activate)
    loads[5].wait()
    for e in exchange[8:10]:
        e.wait_recv()
    rows_end = RowSum(place, part, dbuf, rbuf, r_sem)
    done = []

    def downward(j):
        tower = tower_of(j)
        act = acts[j]
        part[own, j] = jnp.dot(wd[0, tower], act, preferred_element_type=F32).astype(BF16)
        part[oth, j] = jnp.dot(wd[1, tower], act, preferred_element_type=F32).astype(BF16)
        rows_end.pair(j)
        if len(done) >= LAG:
            rows_end.pass_on(done[-LAG])
        done.append(j)

    ring.run(downward)
    for j in done[-LAG:]:
        rows_end.pass_on(j)
    total = rows_end.finish()
    out[...] = (resid[...] + total).astype(BF16)

    ring.end()
    rows_in.end()
    rows_mid.end()
    rows_out.end()
    rows_end.end()
    for e in exchange:
        e.wait_send()
    for k in range(1, NZ):
        j = place.along(k)
        squares_to(k).wait_send()
        q_copy(j).wait_send()
        kv_copy(j).wait_send()
        ssa_copy(j).wait_send()
        kz_copy(k).wait_send()
    for side in (1, -1):
        for k in (1, 2):
            cx(k * side, place.z).wait_send()
        for k in (3, 4):
            cx(k * side, place.along(-2 * side)).wait_send()
    pl.when(place.moved != 0)(kv_copy(place.z).wait_send)
    for k in range(NZ):
        for side in range(2):
            ky_copy(side, k, piece(0, k)).wait_send()
        kr_copy(k, piece(1 + k % 2, k)).wait_send()
    for n in range(4):
        kd_copy(n, kvall.at[sources[n][0], sources[n][1], place.c]).wait_send()


def local(tokens, modality, attn_gain, ffn_gain, w_query, w_keyval, w_out, w_gate, w_up, w_down):
    feats = tokens.shape[1]
    width = w_gate.shape[2]
    kvw = w_keyval.shape[2]
    vmem = pl.BlockSpec(memory_space=pltpu.VMEM)
    hbm = pl.BlockSpec(memory_space=pltpu.HBM)
    smem = pl.BlockSpec(memory_space=pltpu.SMEM)
    dma = pltpu.SemaphoreType.DMA
    rows = (feats, MODAL_BLOCK)
    result = pl.pallas_call(
        layer_kernel,
        out_shape=jax.ShapeDtypeStruct(rows, BF16),
        in_specs=[smem, vmem, vmem, vmem] + [hbm] * 6,
        out_specs=vmem,
        scratch_shapes=[
            pltpu.VMEM((2, NB, *rows), BF16),
            pltpu.VMEM((2, feats), F32),
            pltpu.VMEM((2, feats), F32),
            pltpu.VMEM((2, 2, 2, *rows), F32),
            pltpu.VMEM((2, 2, feats, HD), BF16),
            pltpu.VMEM((2, 2, kvw, feats), BF16),
            pltpu.VMEM((2, 2, feats, HD), BF16),
            pltpu.VMEM((2, 2, feats, width), BF16),
            pltpu.VMEM((2, 2, feats, width), BF16),
            pltpu.VMEM((2, 2, feats, width), BF16),
            pltpu.VMEM((2, 2, 2, width, feats), BF16),
            pltpu.VMEM((NZ, HD, MODAL_BLOCK), BF16),
            pltpu.VMEM((NZ, kvw, MODAL_BLOCK), BF16),
            pltpu.VMEM((NZ, HD, MODAL_BLOCK), BF16),
            pltpu.VMEM((NZ, kvw, MODAL_BLOCK), BF16),
            pltpu.VMEM((NZ, 8, MODAL_BLOCK), F32),
            pltpu.VMEM((NZ, 8, MODAL_BLOCK), F32),
            pltpu.VMEM((kvw, MODAL_BLOCK), BF16),
            pltpu.VMEM((2, 2, 2, NZ, kvw, MODAL_BLOCK), BF16),
            pltpu.VMEM((2 * NZ, MODAL_BLOCK, MODAL_BLOCK), F32),
            pltpu.VMEM((NZ, HD, MODAL_BLOCK), BF16),
            pltpu.VMEM((2, NB, *rows), BF16),
            pltpu.VMEM((NB, *rows), BF16),
            pltpu.VMEM((NB, *rows), BF16),
            pltpu.VMEM(rows, F32),
            pltpu.VMEM(rows, BF16),
            pltpu.VMEM((2, NB, *rows), BF16),
            pltpu.VMEM((NZ, 2, width, MODAL_BLOCK), BF16),
            pltpu.VMEM((2, 4, 2, width, MODAL_BLOCK), BF16),
            pltpu.VMEM((NZ, 8, MODAL_BLOCK), F32),
            pltpu.VMEM((NZ, 8, MODAL_BLOCK), F32),
            pltpu.VMEM((NZ, width, MODAL_BLOCK), BF16),
            pltpu.VMEM((2, NB, *rows), BF16),
            pltpu.VMEM((NB, *rows), BF16),
            pltpu.VMEM((NB, *rows), BF16),
            dma((6,)),
            dma((2, 11)),
            dma((4, NB)),
            dma((2, NZ)),
            dma((2, NZ)),
            dma((2, NZ)),
            dma((2, NZ)),
            dma((2, 2, NZ)),
            dma((2, NZ)),
            dma((2, 4)),
            dma((2, NZ)),
            dma((4, NB)),
            dma((4, NB)),
            dma((2, 2, 4, PARTS)),
            dma((2, NZ)),
            dma((2, 2, 4, PARTS)),
            dma((4, NB)),
        ],
        compiler_params=pltpu.CompilerParams(collective_id=0, has_side_effects=True),
        name="layer",
    )(
        modality,
        tokens.T,
        attn_gain,
        ffn_gain,
        w_query,
        jnp.swapaxes(w_keyval, 1, 2),
        jnp.swapaxes(w_out, 1, 2),
        w_gate,
        w_up,
        jnp.swapaxes(w_down, 1, 2),
    )
    return result.T


def solution(mesh):
    torus = Mesh(mesh.devices.reshape(NX, NYH, 2, 2, NZ), AXES)
    in_specs = (
        P(ROWS, MP),
        P(),
        P(None, MP),
        P(None, MP),
        P(None, MP, ROWS),
        P(None, MP, ROWS),
        P(None, ROWS, MP),
        P(None, MP, ROWS),
        P(None, MP, ROWS),
        P(None, ROWS, MP),
    )
    out_specs = P(ROWS, MP)
    return jax.shard_map(local, mesh=torus, in_specs=in_specs, out_specs=out_specs, check_vma=False)
```
